32 devices in a mesh: dp: 4 (over x, y), sp: 8 (over z, core).
Axes of the slice: x: 2, y: 2, z: 4, core: 2. Of those that a mesh axis runs over, the one named last changes fastest.
Arguments:
- hidden_in: bfloat16 [8192, 3072], P(('dp', 'sp')), parts along dimension 0
- positions: int32 [8192], P(('dp', 'sp')), parts along dimension 0
- g_kv: bfloat16 [3072], replicated
- w_k: bfloat16 [3072, 3072], replicated
- w_v: bfloat16 [3072, 3072], replicated
- g_attn: bfloat16 [2, 3072], replicated
- w_q: bfloat16 [2, 3072, 3072], replicated
- w_o: bfloat16 [2, 32, 96, 3072], replicated
- g_mlp: bfloat16 [2, 3072], replicated
- w_gate: bfloat16 [2, 3072, 8192], replicated
- w_up: bfloat16 [2, 3072, 8192], replicated
- w_down: bfloat16 [2, 8192, 3072], replicated
Outputs:
- output: bfloat16 [8192, 3072], P(('dp', 'sp')), parts along dimension 0
There are 4 independent parts. The reference program is written for one: setup_inputs(seed, part) draws one part's arguments, and reference() takes and returns one part's arrays. A program takes and returns all parts, laid end to end along the dimension named above; an argument that names none is the same for every part.
All inputs are finite; a program needn't handle non-finite values.
Results may differ from the reference program's by a relative error of at most 0.02.
Values are sent between devices in bfloat16 or wider.
A program may use at most 1.75 GiB of HBM per device.

```python
import jax
import jax.numpy as jnp
from jax import lax

D_MODEL = 3072
Q_HEADS = 32
KV_HEADS = 32
HEAD_DIM = 96
FF_DIM = 8192
LAYERS = 2
TOKENS_DEV = 256
SEQ_DEVICES = 8

SEQ_LEN = TOKENS_DEV * SEQ_DEVICES
PIECE_LEN = TOKENS_DEV // 2
GROUP_SIZE = Q_HEADS // KV_HEADS
QUERY_BLOCK = min(64, SEQ_LEN)
NORM_EPS = 1e-6
SCORE_SCALE = HEAD_DIM ** -0.5
OUT_GAIN = 2.0 * (SEQ_LEN / 256.0) ** 0.35


def piece_positions(key):
    pair_ids = jax.random.permutation(key, SEQ_DEVICES).astype(jnp.int32)
    offsets = jnp.arange(PIECE_LEN, dtype=jnp.int32)
    first_half = pair_ids[:, None] * PIECE_LEN + offsets[None, :]
    second_half = (2 * SEQ_DEVICES - 1 - pair_ids)[:, None] * PIECE_LEN + offsets[None, :]
    return jnp.concatenate([first_half, second_half], axis=1).reshape(SEQ_LEN)


def gain_vector(key, shape):
    return (1.0 + 0.3 * jax.random.normal(key, shape, jnp.float32)).astype(jnp.bfloat16)


def scaled_normal(key, shape, scale):
    return (scale * jax.random.normal(key, shape, jnp.float32)).astype(jnp.bfloat16)


def setup_inputs(seed: int = 0, part: int = 0) -> dict:
    part_key = jax.random.fold_in(jax.random.key(seed), part)
    row_key, pos_key = jax.random.split(part_key, 2)
    shared = jax.random.split(jax.random.key(seed + 1), 10)
    qk_scale = 1.4 * D_MODEL ** -0.5
    return {
        'hidden_in': scaled_normal(row_key, (SEQ_LEN, D_MODEL), 1.0),
        'positions': piece_positions(pos_key),
        'g_kv': gain_vector(shared[0], (D_MODEL,)),
        'w_k': scaled_normal(shared[1], (D_MODEL, KV_HEADS * HEAD_DIM), qk_scale),
        'w_v': scaled_normal(shared[2], (D_MODEL, KV_HEADS * HEAD_DIM), D_MODEL ** -0.5),
        'g_attn': gain_vector(shared[3], (LAYERS, D_MODEL)),
        'w_q': scaled_normal(shared[4], (LAYERS, D_MODEL, Q_HEADS * HEAD_DIM), qk_scale),
        'w_o': scaled_normal(shared[5], (LAYERS, Q_HEADS, HEAD_DIM, D_MODEL), OUT_GAIN * (Q_HEADS * HEAD_DIM) ** -0.5),
        'g_mlp': gain_vector(shared[6], (LAYERS, D_MODEL)),
        'w_gate': scaled_normal(shared[7], (LAYERS, D_MODEL, FF_DIM), D_MODEL ** -0.5),
        'w_up': scaled_normal(shared[8], (LAYERS, D_MODEL, FF_DIM), D_MODEL ** -0.5),
        'w_down': scaled_normal(shared[9], (LAYERS, FF_DIM, D_MODEL), 2.0 * FF_DIM ** -0.5),
    }


def rms_norm(rows, gain):
    rows32 = rows.astype(jnp.float32)
    inv_rms = lax.rsqrt(jnp.mean(rows32 * rows32, axis=-1, keepdims=True) + NORM_EPS)
    return (rows32 * inv_rms * gain.astype(jnp.float32)).astype(jnp.bfloat16)


def reference(hidden_in, positions, g_kv, w_k, w_v, g_attn, w_q, w_o, g_mlp, w_gate, w_up, w_down):
    normed = rms_norm(hidden_in, g_kv)
    keys32 = jnp.dot(normed, w_k, preferred_element_type=jnp.float32).astype(jnp.bfloat16).astype(jnp.float32).reshape(SEQ_LEN, KV_HEADS, HEAD_DIM)
    values32 = jnp.dot(normed, w_v, preferred_element_type=jnp.float32).astype(jnp.bfloat16).astype(jnp.float32).reshape(SEQ_LEN, KV_HEADS, HEAD_DIM)
    pos_blocks = positions.reshape(SEQ_LEN // QUERY_BLOCK, QUERY_BLOCK)

    def layer_step(hidden, weights):
        gain_a, wq_layer, wo_layer, gain_m, wg_layer, wu_layer, wd_layer = weights
        queries = jnp.dot(rms_norm(hidden, gain_a), wq_layer, preferred_element_type=jnp.float32).astype(jnp.bfloat16)
        q_blocks = queries.astype(jnp.float32).reshape(SEQ_LEN // QUERY_BLOCK, QUERY_BLOCK, GROUP_SIZE, KV_HEADS, HEAD_DIM)

        def attend(block):
            q_block, q_pos = block
            scores = jnp.einsum('qrgd,kgd->rgqk', q_block, keys32) * SCORE_SCALE
            allowed = positions[None, :] <= q_pos[:, None]
            scores = jnp.where(allowed[None, None], scores, -jnp.inf)
            attn_probs = jax.nn.softmax(scores, axis=-1).astype(jnp.bfloat16).astype(jnp.float32)
            return jnp.einsum('rgqk,kgd->qrgd', attn_probs, values32).astype(jnp.bfloat16)

        attn_out = lax.map(attend, (q_blocks, pos_blocks)).reshape(SEQ_LEN, Q_HEADS * HEAD_DIM)
        attn_proj = jnp.dot(attn_out, wo_layer.reshape(Q_HEADS * HEAD_DIM, D_MODEL), preferred_element_type=jnp.float32).astype(jnp.bfloat16)
        hidden = (hidden.astype(jnp.float32) + attn_proj.astype(jnp.float32)).astype(jnp.bfloat16)
        normed_m = rms_norm(hidden, gain_m)
        gate = jnp.dot(normed_m, wg_layer, preferred_element_type=jnp.float32).astype(jnp.bfloat16)
        upper = jnp.dot(normed_m, wu_layer, preferred_element_type=jnp.float32).astype(jnp.bfloat16)
        mlp_act = (jax.nn.silu(gate.astype(jnp.float32)) * upper.astype(jnp.float32)).astype(jnp.bfloat16)
        down_proj = jnp.dot(mlp_act, wd_layer, preferred_element_type=jnp.float32).astype(jnp.bfloat16)
        hidden = (hidden.astype(jnp.float32) + down_proj.astype(jnp.float32)).astype(jnp.bfloat16)
        return hidden, None

    hidden_out, _ = lax.scan(layer_step, hidden_in, (g_attn, w_q, w_o, g_mlp, w_gate, w_up, w_down))
    return hidden_out
```

```python
import functools

import jax
import jax.numpy as jnp
from jax import lax
from jax.experimental import pallas as pl
from jax.experimental.pallas import tpu as pltpu
from jax.sharding import PartitionSpec as P

NORM_EPS = 1e-6
LOG2_E = 1.4426950408889634
PIECE = 128
ROWS = 2 * PIECE
ZS = 4
SP = 2 * ZS
SEQ = SP * ROWS
HEAD_DIM = 96
HEADS_STEP = 4
LANES_STEP = HEADS_STEP * HEAD_DIM
TILE = 512
W_SLOTS = 8
D_SLOTS = 3
KV_COLS = 768
VMEM_LIMIT = 67_043_328
ANY = pl.BlockSpec(memory_space=pl.ANY)
VMEM = pl.BlockSpec(memory_space=pltpu.VMEM)
SMEM = pl.BlockSpec(memory_space=pltpu.SMEM)


def norm_rows(load, store, gain, rows):
    def block(i, carry):
        for part in range(4):
            at = pl.multiple_of(i * 64 + part * 16, 16)
            rows32 = load(at).astype(jnp.float32)
            inv_rms = lax.rsqrt(jnp.mean(rows32 * rows32, axis=-1, keepdims=True) + NORM_EPS)
            store(at, (rows32 * inv_rms * gain).astype(jnp.bfloat16))
        return carry

    lax.fori_loop(0, rows // 64, block, 0)


def remote_unit(z, step):
    flip = z // 2
    near = jnp.where(flip == 1, ZS - 1 - z, z)
    src_end, half_end = step // 2 + 1, step % 2
    src_mid = jnp.where(step < 4, 2 - 2 * (step % 2), 3)
    half_mid = jnp.where(step < 4, step // 2, step % 2)
    src = jnp.where(near == 0, src_end, src_mid)
    half = jnp.where(near == 0, half_end, half_mid)
    return jnp.where(flip == 1, ZS - 1 - src, src), half


def gather_kernel(x_ref, pos_ref, g_ref, wk_ref, wv_ref, k_out, vt_out, pos_out,
                  wk_buf, wv_buf, xbuf, ubuf, kst, vst, pbuf,
                  w_sem, x_sem, out_sem, recv, send_right, send_left, send_sib, psend, precv):
    sp = lax.axis_index('sp')
    z, core = sp // 2, sp % 2
    other = 1 - core
    sib = sp + 1 - 2 * core
    chunks = wk_buf.shape[0]
    cols = wk_buf.shape[2]

    barrier = pltpu.get_barrier_semaphore()
    for hop in range(1, SP):
        pl.semaphore_signal(barrier, inc=1, device_id={'sp': (sp + hop) % SP}, device_id_type=pl.DeviceIdType.MESH)

    def x_copy(half):
        return pltpu.make_async_copy(x_ref.at[pl.ds(half * PIECE, PIECE), :], xbuf.at[core, z, half], x_sem.at[half])

    def w_copy(n, which):
        src, dst = ((wk_ref, wk_buf), (wv_ref, wv_buf))[which]
        return pltpu.make_async_copy(src.at[:, pl.ds(n * cols, cols)], dst.at[n], w_sem.at[which, n])

    for half in range(2):
        x_copy(half).start()
    for n in range(chunks):
        for which in range(2):
            w_copy(n, which).start()
    pl.semaphore_wait(barrier, SP - 1)

    def pos_send(hop):
        return pltpu.make_async_remote_copy(src_ref=pos_ref, dst_ref=pbuf.at[sp], send_sem=psend.at[hop], recv_sem=precv.at[sp],
                                            device_id={'sp': (sp + hop) % SP}, device_id_type=pl.DeviceIdType.MESH)

    def x_send(lane, src, half, sems, target):
        return pltpu.make_async_remote_copy(src_ref=xbuf.at[lane, src, half], dst_ref=xbuf.at[lane, src, half],
                                            send_sem=sems.at[src, half], recv_sem=recv.at[lane, src, half],
                                            device_id={'sp': target}, device_id_type=pl.DeviceIdType.MESH)

    def goes_right(src):
        return (src <= z) & (z < ZS - 1)

    def goes_left(src):
        return (src >= z) & (z > 0)

    def pass_on(src, half):
        @pl.when(goes_right(src))
        def _():
            x_send(core, src, half, send_right, sp + 2).start()

        @pl.when(goes_left(src))
        def _():
            x_send(core, src, half, send_left, sp - 2).start()

        x_send(core, src, half, send_sib, sib).start()

    for half in range(2):
        x_copy(half).wait()
        pass_on(z, half)
    for hop in range(1, SP):
        pos_send(hop).start()

    gain = g_ref[...].astype(jnp.float32)

    def arrive(step):
        src, half = remote_unit(z, step)
        x_send(core, src, half, send_sib, sib).wait_recv()
        pass_on(src, half)

    middle = (z > 0) & (z < ZS - 1)

    def out_copies(par, n, src, half):
        copies = []
        for lane in range(2):
            slot = (2 * src + lane) * 2 + half
            col = pl.multiple_of(n * cols, 128)
            copies.append(pltpu.make_async_copy(kst.at[par, pl.ds(lane * PIECE, PIECE), :], k_out.at[slot, :, pl.ds(col, cols)], out_sem.at[par, lane]))
            copies.append(pltpu.make_async_copy(vst.at[par, :, pl.ds(lane * PIECE, PIECE)],
                                                vt_out.at[pl.ds(col, cols), pl.ds(pl.multiple_of(slot * PIECE, PIECE), PIECE)], out_sem.at[par, 2 + lane]))
        return copies

    def unit_step(unit, carry):
        more = (unit >= 1) & (unit < 7)

        @pl.when(more & middle)
        def _():
            arrive(unit - 1)

        far_src, far_half = remote_unit(z, jnp.maximum(unit - 2, 0))
        src = jnp.where(unit < 2, z, far_src)
        half = jnp.where(unit < 2, unit, far_half)
        x_send(other, src, half, send_sib, sib).wait_recv()
        for lane in range(2):
            def load(at, lane=lane):
                return xbuf[lane, src, half, pl.ds(at, 16), :]

            def store(at, value, lane=lane):
                ubuf[pl.ds(lane * PIECE + at, 16), :] = value

            norm_rows(load, store, gain, PIECE)

        def chunk_step(n, carry):
            par = (unit * chunks + n) % 2

            @pl.when(unit == 0)
            def _():
                w_copy(n, 0).wait()
                w_copy(n, 1).wait()

            @pl.when(unit * chunks + n >= 2)
            def _():
                for copy in out_copies(par, n, src, half):
                    copy.wait()

            keys = jnp.dot(ubuf[...], wk_buf[n], preferred_element_type=jnp.float32).astype(jnp.bfloat16)
            kst[par] = keys
            values = jnp.dot(ubuf[...], wv_buf[n], preferred_element_type=jnp.float32).astype(jnp.bfloat16)
            vst[par] = values.T
            for copy in out_copies(par, n, src, half):
                copy.start()
            return carry

        lax.fori_loop(0, chunks, chunk_step, 0)

        @pl.when(more & jnp.logical_not(middle))
        def _():
            arrive(unit - 1)

        return carry

    lax.fori_loop(0, 8, unit_step, 0)

    for par in range(2):
        for copy in out_copies(par, 0, 0, 0):
            copy.wait()

    for hop in range(1, SP):
        pos_send(hop).wait_send()
        src = (sp + hop) % SP
        pltpu.make_async_remote_copy(src_ref=pos_ref, dst_ref=pbuf.at[src], send_sem=psend.at[hop], recv_sem=precv.at[src],
                                     device_id={'sp': src}, device_id_type=pl.DeviceIdType.MESH).wait_recv()
    pbuf[sp] = pos_ref[...]
    pos_out[...] = pbuf[...]
    for src in range(ZS):
        for half in range(2):
            @pl.when(goes_right(src))
            def _(src=src, half=half):
                x_send(core, src, half, send_right, sp + 2).wait_send()

            @pl.when(goes_left(src))
            def _(src=src, half=half):
                x_send(core, src, half, send_left, sp - 2).wait_send()

            x_send(core, src, half, send_sib, sib).wait_send()


def gather_kv(rows_in, pos_rows, g_kv, w_k, w_v):
    width = rows_in.shape[1]
    out_width = w_k.shape[1]
    cols = min(KV_COLS, out_width)
    chunks = out_width // cols
    pos_tile = jnp.broadcast_to(pos_rows.reshape(2, 1, PIECE), (2, 4, PIECE)).reshape(8, PIECE)
    return pl.pallas_call(
        gather_kernel,
        out_shape=(jax.ShapeDtypeStruct((2 * SP, PIECE, out_width), jnp.bfloat16),
                   jax.ShapeDtypeStruct((out_width, SEQ), jnp.bfloat16),
                   jax.ShapeDtypeStruct((SP, 8, PIECE), jnp.int32)),
        in_specs=[ANY, VMEM, VMEM, ANY, ANY],
        out_specs=(ANY, ANY, VMEM),
        scratch_shapes=[
            pltpu.VMEM((chunks, width, cols), jnp.bfloat16),
            pltpu.VMEM((chunks, width, cols), jnp.bfloat16),
            pltpu.VMEM((2, ZS, 2, PIECE, width), jnp.bfloat16),
            pltpu.VMEM((ROWS, width), jnp.bfloat16),
            pltpu.VMEM((2, ROWS, cols), jnp.bfloat16),
            pltpu.VMEM((2, cols, ROWS), jnp.bfloat16),
            pltpu.VMEM((SP, 8, PIECE), jnp.int32),
            pltpu.SemaphoreType.DMA((2, chunks)),
            pltpu.SemaphoreType.DMA((2,)),
            pltpu.SemaphoreType.DMA((2, 4)),
            pltpu.SemaphoreType.DMA((2, ZS, 2)),
            pltpu.SemaphoreType.DMA((ZS, 2)),
            pltpu.SemaphoreType.DMA((ZS, 2)),
            pltpu.SemaphoreType.DMA((ZS, 2)),
            pltpu.SemaphoreType.DMA((SP,)),
            pltpu.SemaphoreType.DMA((SP,)),
        ],
        compiler_params=pltpu.CompilerParams(collective_id=0, has_side_effects=True, vmem_limit_bytes=VMEM_LIMIT),
        name='gather_kv',
    )(rows_in, pos_tile, g_kv.reshape(1, width), w_k, w_v)


def layers_kernel(pos_all, qpos_ref, x_ref, k_ref, vt_ref, ga_ref, gm_ref, wq_ref, wo_ref, wg_ref, wu_ref, wd_ref, h_ref,
                  wbuf, dbuf, kbuf, vbuf, qbuf, ubuf, acc, act, where_piece, w_sem, d_sem, kv_sem):
    layers, width, q_width = wq_ref.shape
    ff = wg_ref.shape[2]
    q_tiles, o_tiles, f_tiles = q_width // TILE, width // TILE, ff // TILE
    groups = q_width // LANES_STEP
    o_base = q_tiles
    f_base = q_tiles + o_tiles
    per_layer = f_base + 2 * f_tiles
    w_total, d_total = layers * per_layer, layers * f_tiles
    scale = HEAD_DIM ** -0.5 * LOG2_E

    for slot in range(2 * SP):
        where_piece[pos_all[slot // 2, 4 * (slot % 2), 0] // PIECE] = slot

    def w_src(layer, ref, tile):
        return ref.at[layer, :, pl.ds(pl.multiple_of(tile * TILE, TILE), TILE)]

    def issue_w(s):
        layer, r = s // per_layer, s % per_layer
        slot = s % W_SLOTS

        def go(ref, tile):
            pltpu.make_async_copy(w_src(layer, ref, tile), wbuf.at[slot], w_sem.at[slot]).start()

        pl.when((s < w_total) & (r < o_base))(lambda: go(wq_ref, r))
        pl.when((s < w_total) & (r >= o_base) & (r < f_base))(lambda: go(wo_ref, r - o_base))
        rr = r - f_base
        pl.when((s < w_total) & (r >= f_base) & (rr % 2 == 0))(lambda: go(wg_ref, rr // 2))
        pl.when((s < w_total) & (r >= f_base) & (rr % 2 == 1))(lambda: go(wu_ref, rr // 2))

    def wait_w(s):
        slot = s % W_SLOTS
        pltpu.make_async_copy(w_src(0, wq_ref, 0), wbuf.at[slot], w_sem.at[slot]).wait()
        return slot

    def issue_d(s):
        layer, tile = s // f_tiles, s % f_tiles
        slot = s % D_SLOTS

        @pl.when(s < d_total)
        def _():
            pltpu.make_async_copy(wd_ref.at[layer, pl.ds(pl.multiple_of(tile * TILE, TILE), TILE), :], dbuf.at[slot], d_sem.at[slot]).start()

    def wait_d(s):
        slot = s % D_SLOTS
        pltpu.make_async_copy(wd_ref.at[0, pl.ds(0, TILE), :], dbuf.at[slot], d_sem.at[slot]).wait()
        return slot

    def issue_kv(group):
        par = group % 2
        lane = pl.multiple_of(group * LANES_STEP, 128)
        for piece in range(2 * SP):
            slot = where_piece[piece]
            pltpu.make_async_copy(k_ref.at[slot, :, pl.ds(lane, LANES_STEP)], kbuf.at[par, pl.ds(piece * PIECE, PIECE), :], kv_sem.at[par, 0]).start()
            pltpu.make_async_copy(vt_ref.at[pl.ds(lane, LANES_STEP), pl.ds(pl.multiple_of(slot * PIECE, PIECE), PIECE)],
                                  vbuf.at[par, :, pl.ds(piece * PIECE, PIECE)], kv_sem.at[par, 1]).start()

    def wait_kv(group):
        par = group % 2
        pltpu.make_async_copy(kbuf.at[par], kbuf.at[par], kv_sem.at[par, 0]).wait()
        pltpu.make_async_copy(vbuf.at[par], vbuf.at[par], kv_sem.at[par, 1]).wait()
        return par

    for s in range(q_tiles):
        issue_w(s)
    issue_kv(0)
    for s in range(q_tiles, W_SLOTS):
        issue_w(s)
    for s in range(D_SLOTS):
        issue_d(s)
    h_ref[...] = x_ref[...]

    def load_h(at):
        return h_ref[pl.ds(at, 16), :]

    def store_u(at, value):
        ubuf[pl.ds(at, 16), :] = value

    def cols_of(i):
        return pl.ds(pl.multiple_of(i * TILE, TILE), TILE)

    half_keys = SEQ // 2

    def attend_group(group, carry):
        @pl.when(group + 1 < groups)
        def _():
            issue_kv(group + 1)

        par = wait_kv(group)
        lane = pl.ds(pl.multiple_of(group * LANES_STEP, 128), LANES_STEP)
        q_t = qbuf[:, lane].T
        q_low, q_high = qpos_ref[:, 0:PIECE], qpos_ref[:, PIECE:ROWS]
        rows_of = lax.broadcasted_iota(jnp.int32, (ROWS, ROWS), 0)
        key_pos = lax.broadcasted_iota(jnp.int32, (half_keys, PIECE), 0)
        see_low = key_pos <= q_low
        see_high = key_pos + half_keys <= q_high
        outs = []
        for head in range(HEADS_STEP):
            base = 0 if head < 2 else 128
            start = head * HEAD_DIM - base
            q_head = jnp.where((rows_of >= start) & (rows_of < start + HEAD_DIM), q_t[base:base + ROWS], jnp.zeros((), jnp.bfloat16))
            s_lower = jnp.dot(kbuf[par, 0:half_keys, base:base + ROWS], q_head, preferred_element_type=jnp.float32)
            s_upper = jnp.dot(kbuf[par, half_keys:SEQ, base:base + ROWS], q_head[:, PIECE:], preferred_element_type=jnp.float32)
            s_a = jnp.where(see_low, s_lower[:, :PIECE], -jnp.inf)
            s_b = s_lower[:, PIECE:]
            s_c = jnp.where(see_high, s_upper, -jnp.inf)
            m_a = jnp.max(s_a, axis=0, keepdims=True)
            m_b = jnp.maximum(jnp.max(s_b, axis=0, keepdims=True), jnp.max(s_c, axis=0, keepdims=True))
            e_a = jnp.exp2((s_a - m_a) * scale)
            e_b = jnp.exp2((s_b - m_b) * scale)
            e_c = jnp.exp2((s_c - m_b) * scale)
            l_a = 1.0 / jnp.sum(e_a, axis=0, keepdims=True)
            l_b = 1.0 / (jnp.sum(e_b, axis=0, keepdims=True) + jnp.sum(e_c, axis=0, keepdims=True))
            p_lower = jnp.concatenate([(e_a * l_a).astype(jnp.bfloat16), (e_b * l_b).astype(jnp.bfloat16)], axis=1)
            p_upper = (e_c * l_b).astype(jnp.bfloat16)
            v_t = vbuf[par, head * HEAD_DIM:(head + 1) * HEAD_DIM, :]
            o_lower = jnp.dot(v_t[:, :half_keys], p_lower, preferred_element_type=jnp.float32)
            o_upper = jnp.dot(v_t[:, half_keys:], p_upper, preferred_element_type=jnp.float32)
            outs.append(jnp.concatenate([o_lower[:, :PIECE], o_lower[:, PIECE:] + o_upper], axis=1).astype(jnp.bfloat16))
        qbuf[:, lane] = jnp.concatenate(outs, axis=0).T
        return carry

    def layer_step(layer, carry):
        w0, d0 = layer * per_layer, layer * f_tiles
        norm_rows(load_h, store_u, ga_ref[layer].astype(jnp.float32), ROWS)

        def q_step(i, carry):
            slot = wait_w(w0 + i)
            qbuf[:, cols_of(i)] = jnp.dot(ubuf[...], wbuf[slot], preferred_element_type=jnp.float32).astype(jnp.bfloat16)
            issue_w(w0 + i + W_SLOTS)
            return carry

        lax.fori_loop(0, q_tiles, q_step, 0)
        lax.fori_loop(0, groups, attend_group, 0)

        @pl.when(layer + 1 < layers)
        def _():
            issue_kv(0)

        def o_step(i, carry):
            slot = wait_w(w0 + o_base + i)
            proj = jnp.dot(qbuf[...], wbuf[slot], preferred_element_type=jnp.float32).astype(jnp.bfloat16)
            h_ref[:, cols_of(i)] = (h_ref[:, cols_of(i)].astype(jnp.float32) + proj.astype(jnp.float32)).astype(jnp.bfloat16)
            issue_w(w0 + o_base + i + W_SLOTS)
            return carry

        lax.fori_loop(0, o_tiles, o_step, 0)
        norm_rows(load_h, store_u, gm_ref[layer].astype(jnp.float32), ROWS)
        acc[...] = jnp.zeros_like(acc)

        def up_tiles(f):
            s = w0 + f_base + 2 * f
            slot_g, slot_u = wait_w(s), wait_w(s + 1)
            gate = jnp.dot(ubuf[...], wbuf[slot_g], preferred_element_type=jnp.float32).astype(jnp.bfloat16)
            upper = jnp.dot(ubuf[...], wbuf[slot_u], preferred_element_type=jnp.float32).astype(jnp.bfloat16)
            act[f % 2] = (jax.nn.silu(gate.astype(jnp.float32)) * upper.astype(jnp.float32)).astype(jnp.bfloat16)

        def up_done(f):
            s = w0 + f_base + 2 * f
            issue_w(s + W_SLOTS)
            issue_w(s + 1 + W_SLOTS)

        def down_tile(f, slot):
            acc[...] += jnp.dot(act[f % 2], dbuf[slot], preferred_element_type=jnp.float32)

        up_tiles(0)
        up_done(0)

        def f_step(f, carry):
            slot = wait_d(d0 + f - 1)
            up_tiles(f)
            down_tile(f - 1, slot)
            up_done(f)
            issue_d(d0 + f - 1 + D_SLOTS)
            return carry

        lax.fori_loop(1, f_tiles, f_step, 0)
        last = f_tiles - 1
        slot = wait_d(d0 + last)
        down_tile(last, slot)
        issue_d(d0 + last + D_SLOTS)
        h_ref[...] = (h_ref[...].astype(jnp.float32) + acc[...].astype(jnp.bfloat16).astype(jnp.float32)).astype(jnp.bfloat16)
        return carry

    lax.fori_loop(0, layers, layer_step, 0)


def decoder_layers(rows_in, pos_rows, pos_all, all_k, all_vt, g_attn, w_q, w_o, g_mlp, w_gate, w_up, w_down):
    width = rows_in.shape[1]
    q_width = w_q.shape[2]
    layers = w_q.shape[0]
    return pl.pallas_call(
        layers_kernel,
        out_shape=jax.ShapeDtypeStruct((ROWS, width), jnp.bfloat16),
        in_specs=[SMEM, VMEM, VMEM, ANY, ANY, VMEM, VMEM, ANY, ANY, ANY, ANY, ANY],
        out_specs=VMEM,
        scratch_shapes=[
            pltpu.VMEM((W_SLOTS, width, TILE), jnp.bfloat16),
            pltpu.VMEM((D_SLOTS, TILE, width), jnp.bfloat16),
            pltpu.VMEM((2, SEQ, LANES_STEP), jnp.bfloat16),
            pltpu.VMEM((2, LANES_STEP, SEQ), jnp.bfloat16),
            pltpu.VMEM((ROWS, q_width), jnp.bfloat16),
            pltpu.VMEM((ROWS, width), jnp.bfloat16),
            pltpu.VMEM((ROWS, width), jnp.float32),
            pltpu.VMEM((2, ROWS, TILE), jnp.bfloat16),
            pltpu.SMEM((2 * SP,), jnp.int32),
            pltpu.SemaphoreType.DMA((W_SLOTS,)),
            pltpu.SemaphoreType.DMA((D_SLOTS,)),
            pltpu.SemaphoreType.DMA((2, 2)),
        ],
        compiler_params=pltpu.CompilerParams(vmem_limit_bytes=VMEM_LIMIT),
        name='layers',
    )(pos_all, pos_rows.reshape(1, ROWS), rows_in, all_k, all_vt, g_attn.reshape(layers, 1, width), g_mlp.reshape(layers, 1, width), w_q, w_o.reshape(layers, q_width, width), w_gate, w_up, w_down)


def solution(mesh):
    row_spec = P(('dp', 'sp'), None)
    pos_spec = P(('dp', 'sp'))
    full = P()

    def local_step(rows_in, pos_rows, g_kv, w_k, w_v, g_attn, w_q, w_o, g_mlp, w_gate, w_up, w_down):
        all_k, all_vt, pos_all = gather_kv(rows_in, pos_rows, g_kv, w_k, w_v)
        return decoder_layers(rows_in, pos_rows, pos_all, all_k, all_vt, g_attn, w_q, w_o, g_mlp, w_gate, w_up, w_down)

    return jax.shard_map(local_step, mesh=mesh, in_specs=(row_spec, pos_spec, full, full, full, full, full, full, full, full, full, full), out_specs=row_spec, check_vma=False)
```

```python
import functools

import jax
import jax.numpy as jnp
from jax import lax
from jax.experimental import pallas as pl
from jax.experimental.pallas import tpu as pltpu
from jax.sharding import PartitionSpec as P

NORM_EPS = 1e-6
LOG2_E = 1.4426950408889634
PIECE = 128
ROWS = 2 * PIECE
ZS = 4
SP = 2 * ZS
SEQ = SP * ROWS
HEAD_DIM = 96
HEADS_STEP = 4
LANES_STEP = HEADS_STEP * HEAD_DIM
TILE = 512
W_SLOTS = 7
D_SLOTS = 3
KV_COLS = 768
Q_COLS = 384
VMEM_LIMIT = 67_043_328
ANY = pl.BlockSpec(memory_space=pl.ANY)
VMEM = pl.BlockSpec(memory_space=pltpu.VMEM)
SMEM = pl.BlockSpec(memory_space=pltpu.SMEM)


def norm_rows(load, store, gain, rows):
    def block(i, carry):
        for part in range(4):
            at = pl.multiple_of(i * 64 + part * 16, 16)
            rows32 = load(at).astype(jnp.float32)
            inv_rms = lax.rsqrt(jnp.mean(rows32 * rows32, axis=-1, keepdims=True) + NORM_EPS)
            store(at, (rows32 * inv_rms * gain).astype(jnp.bfloat16))
        return carry

    lax.fori_loop(0, rows // 64, block, 0)


def remote_unit(z, step):
    flip = z // 2
    near = jnp.where(flip == 1, ZS - 1 - z, z)
    src_end, half_end = step // 2 + 1, step % 2
    src_mid = jnp.where(step < 4, 2 - 2 * (step % 2), 3)
    half_mid = jnp.where(step < 4, step // 2, step % 2)
    src = jnp.where(near == 0, src_end, src_mid)
    half = jnp.where(near == 0, half_end, half_mid)
    return jnp.where(flip == 1, ZS - 1 - src, src), half


def gather_kernel(x_ref, pos_ref, g_ref, wk_ref, wv_ref, ga_ref, wq_ref, k_out, vt_out, pos_out, q_out,
                  wk_buf, wv_buf, xbuf, ubuf, kst, vst, pbuf, wq_buf, qst,
                  w_sem, x_sem, out_sem, wq_sem, qst_sem, recv, send_right, send_left, send_sib, psend, precv):
    sp = lax.axis_index('sp')
    z, core = sp // 2, sp % 2
    other = 1 - core
    sib = sp + 1 - 2 * core
    chunks = wk_buf.shape[0]
    cols = wk_buf.shape[2]

    barrier = pltpu.get_barrier_semaphore()
    for hop in range(1, SP):
        pl.semaphore_signal(barrier, inc=1, device_id={'sp': (sp + hop) % SP}, device_id_type=pl.DeviceIdType.MESH)

    def x_copy(half):
        return pltpu.make_async_copy(x_ref.at[pl.ds(half * PIECE, PIECE), :], xbuf.at[core, z, half], x_sem.at[half])

    def w_copy(n, which):
        src, dst = ((wk_ref, wk_buf), (wv_ref, wv_buf))[which]
        return pltpu.make_async_copy(src.at[:, pl.ds(n * cols, cols)], dst.at[n], w_sem.at[which, n])

    for half in range(2):
        x_copy(half).start()
    for n in range(chunks):
        for which in range(2):
            w_copy(n, which).start()
    pl.semaphore_wait(barrier, SP - 1)

    def pos_send(hop):
        return pltpu.make_async_remote_copy(src_ref=pos_ref, dst_ref=pbuf.at[sp], send_sem=psend.at[hop], recv_sem=precv.at[sp],
                                            device_id={'sp': (sp + hop) % SP}, device_id_type=pl.DeviceIdType.MESH)

    def x_send(lane, src, half, sems, target):
        return pltpu.make_async_remote_copy(src_ref=xbuf.at[lane, src, half], dst_ref=xbuf.at[lane, src, half],
                                            send_sem=sems.at[src, half], recv_sem=recv.at[lane, src, half],
                                            device_id={'sp': target}, device_id_type=pl.DeviceIdType.MESH)

    def goes_right(src):
        return (src <= z) & (z < ZS - 1)

    def goes_left(src):
        return (src >= z) & (z > 0)

    def pass_on(src, half):
        @pl.when(goes_right(src))
        def _():
            x_send(core, src, half, send_right, sp + 2).start()

        @pl.when(goes_left(src))
        def _():
            x_send(core, src, half, send_left, sp - 2).start()

        x_send(core, src, half, send_sib, sib).start()

    for half in range(2):
        x_copy(half).wait()
        pass_on(z, half)
    for hop in range(1, SP):
        pos_send(hop).start()

    gain = g_ref[...].astype(jnp.float32).reshape(1, -1)

    def arrive(step):
        src, half = remote_unit(z, step)
        x_send(core, src, half, send_sib, sib).wait_recv()
        pass_on(src, half)

    middle = (z > 0) & (z < ZS - 1)

    def out_copies(par, n, src, half):
        copies = []
        for lane in range(2):
            slot = (2 * src + lane) * 2 + half
            col = pl.multiple_of(n * cols, 128)
            copies.append(pltpu.make_async_copy(kst.at[par, pl.ds(lane * PIECE, PIECE), :], k_out.at[slot, :, pl.ds(col, cols)], out_sem.at[par, lane]))
            copies.append(pltpu.make_async_copy(vst.at[par, :, pl.ds(lane * PIECE, PIECE)],
                                                vt_out.at[pl.ds(col, cols), pl.ds(pl.multiple_of(slot * PIECE, PIECE), PIECE)], out_sem.at[par, 2 + lane]))
        return copies

    def unit_step(unit, carry):
        more = (unit >= 1) & (unit < 7)

        @pl.when(more & middle)
        def _():
            arrive(unit - 1)

        far_src, far_half = remote_unit(z, jnp.maximum(unit - 2, 0))
        src = jnp.where(unit < 2, z, far_src)
        half = jnp.where(unit < 2, unit, far_half)
        x_send(other, src, half, send_sib, sib).wait_recv()
        for lane in range(2):
            def load(at, lane=lane):
                return xbuf[lane, src, half, pl.ds(at, 16), :]

            def store(at, value, lane=lane):
                ubuf[pl.ds(lane * PIECE + at, 16), :] = value

            norm_rows(load, store, gain, PIECE)

        def chunk_step(n, carry):
            par = (unit * chunks + n) % 2

            @pl.when(unit == 0)
            def _():
                w_copy(n, 0).wait()
                w_copy(n, 1).wait()

            @pl.when(unit * chunks + n >= 2)
            def _():
                for copy in out_copies(par, n, src, half):
                    copy.wait()

            keys = jnp.dot(ubuf[...], wk_buf[n], preferred_element_type=jnp.float32).astype(jnp.bfloat16)
            kst[par] = keys
            values = jnp.dot(ubuf[...], wv_buf[n], preferred_element_type=jnp.float32).astype(jnp.bfloat16)
            vst[par] = values.T
            for copy in out_copies(par, n, src, half):
                copy.start()
            return carry

        lax.fori_loop(0, chunks, chunk_step, 0)

        @pl.when(more & jnp.logical_not(middle))
        def _():
            arrive(unit - 1)

        return carry

    def q_copy(i):
        return pltpu.make_async_copy(wq_ref.at[0, :, pl.ds(pl.multiple_of(i * Q_COLS, 128), Q_COLS)], wq_buf.at[i % 2], wq_sem.at[i % 2])

    def q_store(i):
        return pltpu.make_async_copy(qst.at[i % 2], q_out.at[:, pl.ds(pl.multiple_of(i * Q_COLS, 128), Q_COLS)], qst_sem.at[i % 2])

    q_steps = q_out.shape[1] // Q_COLS

    def q_step(i, carry):
        q_copy(i).wait()

        @pl.when(i >= 2)
        def _():
            q_store(i).wait()

        qst[i % 2] = jnp.dot(ubuf[...], wq_buf[i % 2], preferred_element_type=jnp.float32).astype(jnp.bfloat16)
        q_store(i).start()

        @pl.when(i + 2 < q_steps)
        def _():
            q_copy(i + 2).start()

        return carry

    for i in range(2):
        q_copy(i).start()
    lax.fori_loop(0, 2, unit_step, 0)
    gain_q = ga_ref[...].astype(jnp.float32)[0:1]
    for half in range(2):
        def load(at, half=half):
            return xbuf[core, z, half, pl.ds(at, 16), :]

        def store(at, value, half=half):
            ubuf[pl.ds(half * PIECE + at, 16), :] = value

        norm_rows(load, store, gain_q, PIECE)
    lax.fori_loop(0, q_steps, q_step, 0)
    lax.fori_loop(2, 8, unit_step, 0)

    for i in range(2):
        q_store(i).wait()
    for par in range(2):
        for copy in out_copies(par, 0, 0, 0):
            copy.wait()

    for hop in range(1, SP):
        pos_send(hop).wait_send()
        src = (sp + hop) % SP
        pltpu.make_async_remote_copy(src_ref=pos_ref, dst_ref=pbuf.at[src], send_sem=psend.at[hop], recv_sem=precv.at[src],
                                     device_id={'sp': src}, device_id_type=pl.DeviceIdType.MESH).wait_recv()
    pbuf[sp] = pos_ref[...]
    pos_out[...] = pbuf[...]
    for src in range(ZS):
        for half in range(2):
            @pl.when(goes_right(src))
            def _(src=src, half=half):
                x_send(core, src, half, send_right, sp + 2).wait_send()

            @pl.when(goes_left(src))
            def _(src=src, half=half):
                x_send(core, src, half, send_left, sp - 2).wait_send()

            x_send(core, src, half, send_sib, sib).wait_send()


def gather_kv(rows_in, pos_rows, g_kv, w_k, w_v, g_attn, w_q):
    width = rows_in.shape[1]
    out_width = w_k.shape[1]
    cols = min(KV_COLS, out_width)
    chunks = out_width // cols
    pos_tile = jnp.broadcast_to(pos_rows.reshape(2, 1, PIECE), (2, 4, PIECE)).reshape(8, PIECE)
    return pl.pallas_call(
        gather_kernel,
        out_shape=(jax.ShapeDtypeStruct((2 * SP, PIECE, out_width), jnp.bfloat16),
                   jax.ShapeDtypeStruct((out_width, SEQ), jnp.bfloat16),
                   jax.ShapeDtypeStruct((SP, 8, PIECE), jnp.int32),
                   jax.ShapeDtypeStruct((ROWS, w_q.shape[2]), jnp.bfloat16)),
        in_specs=[ANY, VMEM, VMEM, ANY, ANY, VMEM, ANY],
        out_specs=(ANY, ANY, VMEM, ANY),
        scratch_shapes=[
            pltpu.VMEM((chunks, width, cols), jnp.bfloat16),
            pltpu.VMEM((chunks, width, cols), jnp.bfloat16),
            pltpu.VMEM((2, ZS, 2, PIECE, width), jnp.bfloat16),
            pltpu.VMEM((ROWS, width), jnp.bfloat16),
            pltpu.VMEM((2, ROWS, cols), jnp.bfloat16),
            pltpu.VMEM((2, cols, ROWS), jnp.bfloat16),
            pltpu.VMEM((SP, 8, PIECE), jnp.int32),
            pltpu.VMEM((2, width, Q_COLS), jnp.bfloat16),
            pltpu.VMEM((2, ROWS, Q_COLS), jnp.bfloat16),
            pltpu.SemaphoreType.DMA((2, chunks)),
            pltpu.SemaphoreType.DMA((2,)),
            pltpu.SemaphoreType.DMA((2, 4)),
            pltpu.SemaphoreType.DMA((2,)),
            pltpu.SemaphoreType.DMA((2,)),
            pltpu.SemaphoreType.DMA((2, ZS, 2)),
            pltpu.SemaphoreType.DMA((ZS, 2)),
            pltpu.SemaphoreType.DMA((ZS, 2)),
            pltpu.SemaphoreType.DMA((ZS, 2)),
            pltpu.SemaphoreType.DMA((SP,)),
            pltpu.SemaphoreType.DMA((SP,)),
        ],
        compiler_params=pltpu.CompilerParams(collective_id=0, has_side_effects=True, vmem_limit_bytes=VMEM_LIMIT),
        name='gather_kv',
    )(rows_in, pos_tile, g_kv, w_k, w_v, g_attn, w_q)


def layers_kernel(pos_all, qpos_ref, x_ref, k_ref, vt_ref, ga_ref, gm_ref, wq_ref, wo_ref, wg_ref, wu_ref, wd_ref, q0_ref, h_ref,
                  wbuf, dbuf, kbuf, vbuf, qbuf, ubuf, acc, act, hide, s_low, s_up, s_max, where_piece, w_sem, d_sem, k_sem, v_sem, h_sem):
    layers, width, q_width = wq_ref.shape
    ff = wg_ref.shape[2]
    q_tiles, o_tiles, f_tiles = q_width // TILE, width // TILE, ff // TILE
    groups = q_width // LANES_STEP
    o_base = q_tiles
    f_base = q_tiles + o_tiles
    per_layer = f_base + 2 * f_tiles
    w_first, w_total, d_total = q_tiles, layers * per_layer, layers * f_tiles
    scale = HEAD_DIM ** -0.5 * LOG2_E

    for slot in range(2 * SP):
        where_piece[pos_all[slot // 2, 4 * (slot % 2), 0] // PIECE] = slot

    def w_src(layer, ref, tile):
        return ref.at[layer, :, pl.ds(pl.multiple_of(tile * TILE, TILE), TILE)]

    def issue_w(s):
        layer, r = s // per_layer, s % per_layer
        slot = s % W_SLOTS

        def go(ref, tile):
            pltpu.make_async_copy(w_src(layer, ref, tile), wbuf.at[slot], w_sem.at[slot]).start()

        pl.when((s < w_total) & (r < o_base))(lambda: go(wq_ref, r))
        pl.when((s < w_total) & (r >= o_base) & (r < f_base))(lambda: go(wo_ref, r - o_base))
        rr = r - f_base
        pl.when((s < w_total) & (r >= f_base) & (rr % 2 == 0))(lambda: go(wg_ref, rr // 2))
        pl.when((s < w_total) & (r >= f_base) & (rr % 2 == 1))(lambda: go(wu_ref, rr // 2))

    def wait_w(s):
        slot = s % W_SLOTS
        pltpu.make_async_copy(w_src(0, wq_ref, 0), wbuf.at[slot], w_sem.at[slot]).wait()
        return slot

    def issue_d(s):
        layer, tile = s // f_tiles, s % f_tiles
        slot = s % D_SLOTS

        @pl.when(s < d_total)
        def _():
            pltpu.make_async_copy(wd_ref.at[layer, pl.ds(pl.multiple_of(tile * TILE, TILE), TILE), :], dbuf.at[slot], d_sem.at[slot]).start()

    def wait_d(s):
        slot = s % D_SLOTS
        pltpu.make_async_copy(wd_ref.at[0, pl.ds(0, TILE), :], dbuf.at[slot], d_sem.at[slot]).wait()
        return slot

    def issue_k(turn):
        lane = pl.multiple_of(turn % groups * LANES_STEP, 128)
        buf = turn % 3
        for piece in range(2 * SP):
            pltpu.make_async_copy(k_ref.at[where_piece[piece], :, pl.ds(lane, LANES_STEP)], kbuf.at[buf, pl.ds(piece * PIECE, PIECE), :], k_sem.at[buf]).start()

    def issue_v(turn):
        lane = pl.multiple_of(turn % groups * LANES_STEP, 128)
        buf = turn % 2
        for piece in range(2 * SP):
            col = pl.multiple_of(where_piece[piece] * PIECE, PIECE)
            pltpu.make_async_copy(vt_ref.at[pl.ds(lane, LANES_STEP), pl.ds(col, PIECE)], vbuf.at[buf, :, pl.ds(piece * PIECE, PIECE)], v_sem.at[buf]).start()

    def wait_k(turn):
        buf = turn % 3
        pltpu.make_async_copy(kbuf.at[buf], kbuf.at[buf], k_sem.at[buf]).wait()

    def wait_v(turn):
        buf = turn % 2
        pltpu.make_async_copy(vbuf.at[buf], vbuf.at[buf], v_sem.at[buf]).wait()

    issue_k(0)
    issue_v(0)
    issue_k(1)
    for s in range(w_first, w_first + W_SLOTS):
        issue_w(s)
    for s in range(D_SLOTS):
        issue_d(s)
    load_q = pltpu.make_async_copy(q0_ref, qbuf, h_sem.at[0])
    load_x = pltpu.make_async_copy(x_ref, h_ref, h_sem.at[1])
    load_q.start()
    load_x.start()

    def load_h(at):
        return h_ref[pl.ds(at, 16), :]

    def store_u(at, value):
        ubuf[pl.ds(at, 16), :] = value

    def gain_of(ref, layer):
        gains = ref[...].astype(jnp.float32)
        gain = gains[0:1]
        for other in range(1, layers):
            gain = jnp.where(layer == other, gains[other:other + 1], gain)
        return gain

    def cols_of(i):
        return pl.ds(pl.multiple_of(i * TILE, TILE), TILE)

    half_keys = SEQ // 2
    key_pos = lax.broadcasted_iota(jnp.int32, (half_keys, PIECE), 0)
    hide[0:half_keys] = jnp.where(key_pos <= qpos_ref[:, 0:PIECE], 0.0, -jnp.inf)
    hide[half_keys:SEQ] = jnp.where(key_pos + half_keys <= qpos_ref[:, PIECE:ROWS], 0.0, -jnp.inf)

    def scores(turn, pair):
        buf = turn % 3
        base = 128 * pair
        window_at = pl.multiple_of(turn % groups * LANES_STEP + base, 128)
        window = qbuf[:, pl.ds(window_at, ROWS)].T
        rows_of = lax.broadcasted_iota(jnp.int32, (ROWS, ROWS), 0)
        heads = []
        for i in range(2):
            start = HEAD_DIM * (2 * pair + i) - base
            heads.append(jnp.where((rows_of >= start) & (rows_of < start + HEAD_DIM), window, jnp.zeros((), jnp.bfloat16)))
        both = jnp.concatenate([heads[0][:, PIECE:], heads[1][:, PIECE:]], axis=1)
        upper = jnp.dot(kbuf[buf, half_keys:SEQ, base:base + ROWS], both, preferred_element_type=jnp.float32)
        for i in range(2):
            lower = jnp.dot(kbuf[buf, 0:half_keys, base:base + ROWS], heads[i], preferred_element_type=jnp.float32)
            s_a = lower[:, :PIECE] + hide[0:half_keys]
            s_b = lower[:, PIECE:]
            s_c = upper[:, i * PIECE:(i + 1) * PIECE] + hide[half_keys:SEQ]
            s_low[pair, i, :, 0:PIECE] = s_a
            s_low[pair, i, :, PIECE:ROWS] = s_b
            s_up[pair, i] = s_c
            m_a = jnp.max(s_a, axis=0, keepdims=True)
            m_b = jnp.maximum(jnp.max(s_b, axis=0, keepdims=True), jnp.max(s_c, axis=0, keepdims=True))
            s_max[pair, i] = jnp.broadcast_to(jnp.concatenate([m_a, m_b], axis=1), (8, ROWS))

    def attend(turn, pair):
        buf = turn % 2
        p_lowers, p_uppers, inverses = [], [], []
        for i in range(2):
            m_a, m_b = s_max[pair, i, 0:1, 0:PIECE], s_max[pair, i, 0:1, PIECE:ROWS]
            e_a = jnp.exp2((s_low[pair, i, :, 0:PIECE] - m_a) * scale)
            e_b = jnp.exp2((s_low[pair, i, :, PIECE:ROWS] - m_b) * scale)
            e_c = jnp.exp2((s_up[pair, i] - m_b) * scale)
            l_a = jnp.sum(e_a, axis=0, keepdims=True)
            l_b = jnp.sum(e_b, axis=0, keepdims=True) + jnp.sum(e_c, axis=0, keepdims=True)
            p_lowers.append(jnp.concatenate([e_a.astype(jnp.bfloat16), e_b.astype(jnp.bfloat16)], axis=1))
            p_uppers.append(e_c.astype(jnp.bfloat16))
            inverses.append(1.0 / jnp.concatenate([l_a, l_b], axis=1))
        top = 2 * pair * HEAD_DIM
        o_upper = jnp.dot(vbuf[buf, top:top + 2 * HEAD_DIM, half_keys:SEQ], jnp.concatenate(p_uppers, axis=1), preferred_element_type=jnp.float32)
        outs = []
        for i in range(2):
            o_lower = jnp.dot(vbuf[buf, top + i * HEAD_DIM:top + (i + 1) * HEAD_DIM, 0:half_keys], p_lowers[i], preferred_element_type=jnp.float32)
            mine = o_upper[i * HEAD_DIM:(i + 1) * HEAD_DIM, i * PIECE:(i + 1) * PIECE]
            o_t = jnp.concatenate([o_lower[:, :PIECE], o_lower[:, PIECE:] + mine], axis=1)
            outs.append((o_t * inverses[i]).astype(jnp.bfloat16))
        return outs

    def attend_group(turn, carry):
        wait_k(turn + 1)
        wait_v(turn)
        issue_k(turn + 2)
        issue_v(turn + 1)
        scores(turn, 1)
        outs = attend(turn, 0)
        scores(turn + 1, 0)
        outs += attend(turn, 1)
        lane = pl.ds(pl.multiple_of(turn % groups * LANES_STEP, 128), LANES_STEP)
        ubuf[:, lane] = jnp.concatenate(outs, axis=0).T
        return carry

    load_q.wait()
    load_x.wait()
    wait_k(0)

    def layer_step(layer, carry):
        w0, d0 = layer * per_layer, layer * f_tiles

        def q_step(i, carry):
            slot = wait_w(w0 + i)
            qbuf[:, cols_of(i)] = jnp.dot(ubuf[...], wbuf[slot], preferred_element_type=jnp.float32).astype(jnp.bfloat16)
            issue_w(w0 + i + W_SLOTS)
            return carry

        @pl.when(layer > 0)
        def _():
            norm_rows(load_h, store_u, gain_of(ga_ref, layer), ROWS)
            lax.fori_loop(0, q_tiles, q_step, 0)

        first = layer * groups
        scores(first, 0)
        lax.fori_loop(first, first + groups, attend_group, 0)

        def o_step(i, carry):
            slot = wait_w(w0 + o_base + i)
            proj = jnp.dot(ubuf[...], wbuf[slot], preferred_element_type=jnp.float32).astype(jnp.bfloat16)
            h_ref[:, cols_of(i)] = (h_ref[:, cols_of(i)].astype(jnp.float32) + proj.astype(jnp.float32)).astype(jnp.bfloat16)
            issue_w(w0 + o_base + i + W_SLOTS)
            return carry

        lax.fori_loop(0, o_tiles, o_step, 0)
        norm_rows(load_h, store_u, gain_of(gm_ref, layer), ROWS)
        acc[...] = jnp.zeros_like(acc)

        def up_tiles(f):
            s = w0 + f_base + 2 * f
            slot_g, slot_u = wait_w(s), wait_w(s + 1)
            gate = jnp.dot(ubuf[...], wbuf[slot_g], preferred_element_type=jnp.float32).astype(jnp.bfloat16)
            upper = jnp.dot(ubuf[...], wbuf[slot_u], preferred_element_type=jnp.float32).astype(jnp.bfloat16)
            act[f % 2] = (jax.nn.silu(gate.astype(jnp.float32)) * upper.astype(jnp.float32)).astype(jnp.bfloat16)

        def up_done(f):
            s = w0 + f_base + 2 * f
            issue_w(s + W_SLOTS)
            issue_w(s + 1 + W_SLOTS)

        def down_tile(f, slot):
            acc[...] += jnp.dot(act[f % 2], dbuf[slot], preferred_element_type=jnp.float32)

        up_tiles(0)
        up_done(0)

        def f_step(f, carry):
            slot = wait_d(d0 + f - 1)
            up_tiles(f)
            down_tile(f - 1, slot)
            up_done(f)
            issue_d(d0 + f - 1 + D_SLOTS)
            return carry

        lax.fori_loop(1, f_tiles, f_step, 0)
        last = f_tiles - 1
        slot = wait_d(d0 + last)
        down_tile(last, slot)
        issue_d(d0 + last + D_SLOTS)
        h_ref[...] = (h_ref[...].astype(jnp.float32) + acc[...].astype(jnp.bfloat16).astype(jnp.float32)).astype(jnp.bfloat16)
        return carry

    lax.fori_loop(0, layers, layer_step, 0)
    wait_v(layers * groups)
    wait_k(layers * groups + 1)


def decoder_layers(rows_in, q_first, pos_rows, pos_all, all_k, all_vt, g_attn, w_q, w_o, g_mlp, w_gate, w_up, w_down):
    width = rows_in.shape[1]
    q_width = w_q.shape[2]
    layers = w_q.shape[0]
    return pl.pallas_call(
        layers_kernel,
        out_shape=jax.ShapeDtypeStruct((ROWS, width), jnp.bfloat16),
        in_specs=[SMEM, VMEM, ANY, ANY, ANY, VMEM, VMEM, ANY, ANY, ANY, ANY, ANY, ANY],
        out_specs=VMEM,
        scratch_shapes=[
            pltpu.VMEM((W_SLOTS, width, TILE), jnp.bfloat16),
            pltpu.VMEM((D_SLOTS, TILE, width), jnp.bfloat16),
            pltpu.VMEM((3, SEQ, LANES_STEP), jnp.bfloat16),
            pltpu.VMEM((2, LANES_STEP, SEQ), jnp.bfloat16),
            pltpu.VMEM((ROWS, q_width), jnp.bfloat16),
            pltpu.VMEM((ROWS, width), jnp.bfloat16),
            pltpu.VMEM((ROWS, width), jnp.float32),
            pltpu.VMEM((2, ROWS, TILE), jnp.bfloat16),
            pltpu.VMEM((SEQ, PIECE), jnp.float32),
            pltpu.VMEM((2, 2, SEQ // 2, ROWS), jnp.float32),
            pltpu.VMEM((2, 2, SEQ // 2, PIECE), jnp.float32),
            pltpu.VMEM((2, 2, 8, ROWS), jnp.float32),
            pltpu.SMEM((2 * SP,), jnp.int32),
            pltpu.SemaphoreType.DMA((W_SLOTS,)),
            pltpu.SemaphoreType.DMA((D_SLOTS,)),
            pltpu.SemaphoreType.DMA((3,)),
            pltpu.SemaphoreType.DMA((2,)),
            pltpu.SemaphoreType.DMA((2,)),
        ],
        compiler_params=pltpu.CompilerParams(vmem_limit_bytes=VMEM_LIMIT),
        name='layers',
    )(pos_all, pos_rows.reshape(1, ROWS), rows_in, all_k, all_vt, g_attn, g_mlp, w_q, w_o.reshape(layers, q_width, width), w_gate, w_up, w_down, q_first)


def solution(mesh):
    row_spec = P(('dp', 'sp'), None)
    pos_spec = P(('dp', 'sp'))
    full = P()

    def local_step(rows_in, pos_rows, g_kv, w_k, w_v, g_attn, w_q, w_o, g_mlp, w_gate, w_up, w_down):
        all_k, all_vt, pos_all, q_first = gather_kv(rows_in, pos_rows, g_kv, w_k, w_v, g_attn, w_q)
        return decoder_layers(rows_in, q_first, pos_rows, pos_all, all_k, all_vt, g_attn, w_q, w_o, g_mlp, w_gate, w_up, w_down)

    return jax.shard_map(local_step, mesh=mesh, in_specs=(row_spec, pos_spec, full, full, full, full, full, full, full, full, full, full), out_specs=row_spec, check_vma=False)
```

```python
import functools

import jax
import jax.numpy as jnp
from jax import lax
from jax.experimental import pallas as pl
from jax.experimental.pallas import tpu as pltpu
from jax.sharding import PartitionSpec as P

NORM_EPS = 1e-6
LOG2_E = 1.4426950408889634
PIECE = 128
ROWS = 2 * PIECE
ZS = 4
SP = 2 * ZS
SEQ = SP * ROWS
HEAD_DIM = 96
HEADS_STEP = 4
LANES_STEP = HEADS_STEP * HEAD_DIM
TILE = 512
W_SLOTS = 7
D_SLOTS = 3
KV_COLS = 768
Q_COLS = 512
VMEM_LIMIT = 67_043_328
ANY = pl.BlockSpec(memory_space=pl.ANY)
VMEM = pl.BlockSpec(memory_space=pltpu.VMEM)
SMEM = pl.BlockSpec(memory_space=pltpu.SMEM)


def norm_rows(load, store, gain, rows):
    def block(i, carry):
        for part in range(4):
            at = pl.multiple_of(i * 64 + part * 16, 16)
            rows32 = load(at).astype(jnp.float32)
            inv_rms = lax.rsqrt(jnp.mean(rows32 * rows32, axis=-1, keepdims=True) + NORM_EPS)
            store(at, (rows32 * inv_rms * gain).astype(jnp.bfloat16))
        return carry

    lax.fori_loop(0, rows // 64, block, 0)


def remote_unit(z, step):
    flip = z // 2
    near = jnp.where(flip == 1, ZS - 1 - z, z)
    src_end, half_end = step // 2 + 1, step % 2
    src_mid = jnp.where(step < 4, 2 - 2 * (step % 2), 3)
    half_mid = jnp.where(step < 4, step // 2, step % 2)
    src = jnp.where(near == 0, src_end, src_mid)
    half = jnp.where(near == 0, half_end, half_mid)
    return jnp.where(flip == 1, ZS - 1 - src, src), half


def gather_kernel(x_ref, pos_ref, g_ref, wk_ref, wv_ref, ga_ref, wq_ref, k_out, vt_out, pos_out, q_out,
                  wk_buf, wv_buf, xbuf, ubuf, kst, vst, pbuf, wq_buf, qst,
                  w_sem, x_sem, out_sem, wq_sem, qst_sem, recv, send_right, send_left, send_sib, psend, precv):
    sp = lax.axis_index('sp')
    z, core = sp // 2, sp % 2
    other = 1 - core
    sib = sp + 1 - 2 * core
    chunks = wk_buf.shape[0]
    cols = wk_buf.shape[2]

    barrier = pltpu.get_barrier_semaphore()
    for hop in range(1, SP):
        pl.semaphore_signal(barrier, inc=1, device_id={'sp': (sp + hop) % SP}, device_id_type=pl.DeviceIdType.MESH)

    def x_copy(half):
        return pltpu.make_async_copy(x_ref.at[pl.ds(half * PIECE, PIECE), :], xbuf.at[core, z, half], x_sem.at[half])

    def w_copy(n, which):
        src, dst = ((wk_ref, wk_buf), (wv_ref, wv_buf))[which]
        return pltpu.make_async_copy(src.at[:, pl.ds(n * cols, cols)], dst.at[n], w_sem.at[which, n])

    for half in range(2):
        x_copy(half).start()
    for n in range(chunks):
        for which in range(2):
            w_copy(n, which).start()
    pl.semaphore_wait(barrier, SP - 1)

    def pos_send(hop):
        return pltpu.make_async_remote_copy(src_ref=pos_ref, dst_ref=pbuf.at[sp], send_sem=psend.at[hop], recv_sem=precv.at[sp],
                                            device_id={'sp': (sp + hop) % SP}, device_id_type=pl.DeviceIdType.MESH)

    def x_send(lane, src, half, sems, target):
        return pltpu.make_async_remote_copy(src_ref=xbuf.at[lane, src, half], dst_ref=xbuf.at[lane, src, half],
                                            send_sem=sems.at[src, half], recv_sem=recv.at[lane, src, half],
                                            device_id={'sp': target}, device_id_type=pl.DeviceIdType.MESH)

    def goes_right(src):
        return (src <= z) & (z < ZS - 1)

    def goes_left(src):
        return (src >= z) & (z > 0)

    def pass_on(src, half):
        @pl.when(goes_right(src))
        def _():
            x_send(core, src, half, send_right, sp + 2).start()

        @pl.when(goes_left(src))
        def _():
            x_send(core, src, half, send_left, sp - 2).start()

        x_send(core, src, half, send_sib, sib).start()

    for half in range(2):
        x_copy(half).wait()
        pass_on(z, half)
    for hop in range(1, SP):
        pos_send(hop).start()

    gain = g_ref[...].astype(jnp.float32).reshape(1, -1)

    def arrive(step):
        src, half = remote_unit(z, step)
        x_send(core, src, half, send_sib, sib).wait_recv()
        pass_on(src, half)

    middle = (z > 0) & (z < ZS - 1)

    def out_copies(par, n, src, half):
        copies = []
        for lane in range(2):
            slot = (2 * src + lane) * 2 + half
            col = pl.multiple_of(n * cols, 128)
            copies.append(pltpu.make_async_copy(kst.at[par, pl.ds(lane * PIECE, PIECE), :], k_out.at[slot, :, pl.ds(col, cols)], out_sem.at[par, lane]))
            copies.append(pltpu.make_async_copy(vst.at[par, :, pl.ds(lane * PIECE, PIECE)],
                                                vt_out.at[pl.ds(col, cols), pl.ds(pl.multiple_of(slot * PIECE, PIECE), PIECE)], out_sem.at[par, 2 + lane]))
        return copies

    def unit_step(unit, carry):
        @pl.when(middle & ((unit == 1) | (unit == 2)))
        def _():
            arrive(2 * unit - 2)
            arrive(2 * unit - 1)

        @pl.when(middle & ((unit == 3) | (unit == 5)))
        def _():
            arrive(4 + unit // 5)

        far_src, far_half = remote_unit(z, jnp.maximum(unit - 2, 0))
        src = jnp.where(unit < 2, z, far_src)
        half = jnp.where(unit < 2, unit, far_half)
        x_send(other, src, half, send_sib, sib).wait_recv()
        for lane in range(2):
            def load(at, lane=lane):
                return xbuf[lane, src, half, pl.ds(at, 16), :]

            def store(at, value, lane=lane):
                ubuf[pl.ds(lane * PIECE + at, 16), :] = value

            norm_rows(load, store, gain, PIECE)

        def chunk_step(n, carry):
            par = (unit * chunks + n) % 2

            @pl.when(unit == 0)
            def _():
                w_copy(n, 0).wait()
                w_copy(n, 1).wait()

            @pl.when(unit * chunks + n >= 2)
            def _():
                for copy in out_copies(par, n, src, half):
                    copy.wait()

            keys = jnp.dot(ubuf[...], wk_buf[n], preferred_element_type=jnp.float32).astype(jnp.bfloat16)
            kst[par] = keys
            values = jnp.dot(ubuf[...], wv_buf[n], preferred_element_type=jnp.float32).astype(jnp.bfloat16)
            vst[par] = values.T
            for copy in out_copies(par, n, src, half):
                copy.start()
            return carry

        lax.fori_loop(0, chunks, chunk_step, 0)

        @pl.when((unit >= 1) & (unit < 7) & jnp.logical_not(middle))
        def _():
            arrive(unit - 1)

        return carry

    def q_copy(i):
        return pltpu.make_async_copy(wq_ref.at[0, :, pl.ds(pl.multiple_of(i * Q_COLS, 128), Q_COLS)], wq_buf.at[i % 2], wq_sem.at[i % 2])

    def q_store(i):
        return pltpu.make_async_copy(qst.at[i % 2], q_out.at[:, pl.ds(pl.multiple_of(i * Q_COLS, 128), Q_COLS)], qst_sem.at[i % 2])

    q_steps = q_out.shape[1] // Q_COLS

    def q_step(i, carry):
        q_copy(i).wait()

        @pl.when(i >= 2)
        def _():
            q_store(i).wait()

        qst[i % 2] = jnp.dot(ubuf[...], wq_buf[i % 2], preferred_element_type=jnp.float32).astype(jnp.bfloat16)
        q_store(i).start()

        @pl.when(i + 2 < q_steps)
        def _():
            q_copy(i + 2).start()

        return carry

    for i in range(2):
        q_copy(i).start()
    lax.fori_loop(0, 2, unit_step, 0)
    gain_q = ga_ref[...].astype(jnp.float32)[0:1]
    for half in range(2):
        def load(at, half=half):
            return xbuf[core, z, half, pl.ds(at, 16), :]

        def store(at, value, half=half):
            ubuf[pl.ds(half * PIECE + at, 16), :] = value

        norm_rows(load, store, gain_q, PIECE)
    lax.fori_loop(0, q_steps, q_step, 0)
    lax.fori_loop(2, 8, unit_step, 0)

    for i in range(2):
        q_store(i).wait()
    for par in range(2):
        for copy in out_copies(par, 0, 0, 0):
            copy.wait()

    for hop in range(1, SP):
        pos_send(hop).wait_send()
        src = (sp + hop) % SP
        pltpu.make_async_remote_copy(src_ref=pos_ref, dst_ref=pbuf.at[src], send_sem=psend.at[hop], recv_sem=precv.at[src],
                                     device_id={'sp': src}, device_id_type=pl.DeviceIdType.MESH).wait_recv()
    pbuf[sp] = pos_ref[...]
    pos_out[...] = pbuf[...]
    for src in range(ZS):
        for half in range(2):
            @pl.when(goes_right(src))
            def _(src=src, half=half):
                x_send(core, src, half, send_right, sp + 2).wait_send()

            @pl.when(goes_left(src))
            def _(src=src, half=half):
                x_send(core, src, half, send_left, sp - 2).wait_send()

            x_send(core, src, half, send_sib, sib).wait_send()


def gather_kv(rows_in, pos_rows, g_kv, w_k, w_v, g_attn, w_q):
    width = rows_in.shape[1]
    out_width = w_k.shape[1]
    cols = min(KV_COLS, out_width)
    chunks = out_width // cols
    pos_tile = jnp.broadcast_to(pos_rows.reshape(2, 1, PIECE), (2, 4, PIECE)).reshape(8, PIECE)
    return pl.pallas_call(
        gather_kernel,
        out_shape=(jax.ShapeDtypeStruct((2 * SP, PIECE, out_width), jnp.bfloat16),
                   jax.ShapeDtypeStruct((out_width, SEQ), jnp.bfloat16),
                   jax.ShapeDtypeStruct((SP, 8, PIECE), jnp.int32),
                   jax.ShapeDtypeStruct((ROWS, w_q.shape[2]), jnp.bfloat16)),
        in_specs=[ANY, VMEM, VMEM, ANY, ANY, VMEM, ANY],
        out_specs=(ANY, ANY, VMEM, ANY),
        scratch_shapes=[
            pltpu.VMEM((chunks, width, cols), jnp.bfloat16),
            pltpu.VMEM((chunks, width, cols), jnp.bfloat16),
            pltpu.VMEM((2, ZS, 2, PIECE, width), jnp.bfloat16),
            pltpu.VMEM((ROWS, width), jnp.bfloat16),
            pltpu.VMEM((2, ROWS, cols), jnp.bfloat16),
            pltpu.VMEM((2, cols, ROWS), jnp.bfloat16),
            pltpu.VMEM((SP, 8, PIECE), jnp.int32),
            pltpu.VMEM((2, width, Q_COLS), jnp.bfloat16),
            pltpu.VMEM((2, ROWS, Q_COLS), jnp.bfloat16),
            pltpu.SemaphoreType.DMA((2, chunks)),
            pltpu.SemaphoreType.DMA((2,)),
            pltpu.SemaphoreType.DMA((2, 4)),
            pltpu.SemaphoreType.DMA((2,)),
            pltpu.SemaphoreType.DMA((2,)),
            pltpu.SemaphoreType.DMA((2, ZS, 2)),
            pltpu.SemaphoreType.DMA((ZS, 2)),
            pltpu.SemaphoreType.DMA((ZS, 2)),
            pltpu.SemaphoreType.DMA((ZS, 2)),
            pltpu.SemaphoreType.DMA((SP,)),
            pltpu.SemaphoreType.DMA((SP,)),
        ],
        compiler_params=pltpu.CompilerParams(collective_id=0, has_side_effects=True, vmem_limit_bytes=VMEM_LIMIT),
        name='gather_kv',
    )(rows_in, pos_tile, g_kv, w_k, w_v, g_attn, w_q)


def layers_kernel(pos_all, qpos_ref, x_ref, k_ref, vt_ref, ga_ref, gm_ref, wq_ref, wo_ref, wg_ref, wu_ref, wd_ref, q0_ref, h_ref,
                  wbuf, dbuf, kbuf, vbuf, qbuf, ubuf, acc, act_new, act_old, hide, s_low, s_up, s_max, where_piece, w_sem, d_sem, k_sem, v_sem, h_sem):
    layers, width, q_width = wq_ref.shape
    ff = wg_ref.shape[2]
    q_tiles, o_tiles, f_tiles = q_width // TILE, width // TILE, ff // TILE
    groups = q_width // LANES_STEP
    o_base = q_tiles
    q_pack, o_pack = 2 - q_tiles % 2, 2 - o_tiles % 2
    f_base = q_tiles + o_tiles
    per_layer = f_base + 2 * f_tiles
    w_first, w_total, d_total = q_tiles, layers * per_layer, layers * f_tiles
    scale = HEAD_DIM ** -0.5 * LOG2_E

    for slot in range(2 * SP):
        where_piece[pos_all[slot // 2, 4 * (slot % 2), 0] // PIECE] = slot

    def w_src(layer, ref, tile):
        return ref.at[layer, :, pl.ds(pl.multiple_of(tile * TILE, TILE), TILE)]

    def issue_w(s):
        layer, r = s // per_layer, s % per_layer
        slot = s % W_SLOTS

        def go(ref, tile):
            pltpu.make_async_copy(w_src(layer, ref, tile), wbuf.at[slot], w_sem.at[slot]).start(priority=1)

        pl.when((s < w_total) & (r < o_base))(lambda: go(wq_ref, r))
        pl.when((s < w_total) & (r >= o_base) & (r < f_base))(lambda: go(wo_ref, r - o_base))
        rr = r - f_base
        pl.when((s < w_total) & (r >= f_base) & (rr % 2 == 0))(lambda: go(wg_ref, rr // 2))
        pl.when((s < w_total) & (r >= f_base) & (rr % 2 == 1))(lambda: go(wu_ref, rr // 2))

    def wait_w(s):
        slot = s % W_SLOTS
        pltpu.make_async_copy(w_src(0, wq_ref, 0), wbuf.at[slot], w_sem.at[slot]).wait()
        return slot

    def issue_d(s):
        layer, tile = s // f_tiles, s % f_tiles
        slot = s % D_SLOTS

        @pl.when(s < d_total)
        def _():
            pltpu.make_async_copy(wd_ref.at[layer, pl.ds(pl.multiple_of(tile * TILE, TILE), TILE), :], dbuf.at[slot], d_sem.at[slot]).start(priority=1)

    def wait_d(s):
        slot = s % D_SLOTS
        pltpu.make_async_copy(wd_ref.at[0, pl.ds(0, TILE), :], dbuf.at[slot], d_sem.at[slot]).wait()
        return slot

    def issue_k(turn):
        lane = pl.multiple_of(turn % groups * LANES_STEP, 128)
        buf = turn % 3
        for piece in range(2 * SP):
            pltpu.make_async_copy(k_ref.at[where_piece[piece], :, pl.ds(lane, LANES_STEP)], kbuf.at[buf, pl.ds(piece * PIECE, PIECE), :], k_sem.at[buf]).start()

    def issue_v(turn):
        lane = pl.multiple_of(turn % groups * LANES_STEP, 128)
        buf = turn % 2
        for piece in range(2 * SP):
            col = pl.multiple_of(where_piece[piece] * PIECE, PIECE)
            pltpu.make_async_copy(vt_ref.at[pl.ds(lane, LANES_STEP), pl.ds(col, PIECE)], vbuf.at[buf, :, pl.ds(piece * PIECE, PIECE)], v_sem.at[buf]).start()

    def wait_k(turn):
        buf = turn % 3
        pltpu.make_async_copy(kbuf.at[buf], kbuf.at[buf], k_sem.at[buf]).wait()

    def wait_v(turn):
        buf = turn % 2
        pltpu.make_async_copy(vbuf.at[buf], vbuf.at[buf], v_sem.at[buf]).wait()

    issue_k(0)
    issue_v(0)
    issue_k(1)
    for s in range(w_first, w_first + W_SLOTS):
        issue_w(s)
    for s in range(D_SLOTS):
        issue_d(s)
    load_q = pltpu.make_async_copy(q0_ref, qbuf, h_sem.at[0])
    load_x = pltpu.make_async_copy(x_ref, h_ref, h_sem.at[1])
    load_q.start()
    load_x.start()

    def load_h(at):
        return h_ref[pl.ds(at, 16), :]

    def store_u(at, value):
        ubuf[pl.ds(at, 16), :] = value

    def gain_of(ref, layer):
        gains = ref[...].astype(jnp.float32)
        gain = gains[0:1]
        for other in range(1, layers):
            gain = jnp.where(layer == other, gains[other:other + 1], gain)
        return gain

    def cols_of(i):
        return pl.ds(pl.multiple_of(i * TILE, TILE), TILE)

    half_keys = SEQ // 2
    key_pos = lax.broadcasted_iota(jnp.int32, (half_keys, PIECE), 0)
    hide[0:half_keys] = jnp.where(key_pos <= qpos_ref[:, 0:PIECE], 0.0, -jnp.inf)
    hide[half_keys:SEQ] = jnp.where(key_pos + half_keys <= qpos_ref[:, PIECE:ROWS], 0.0, -jnp.inf)

    def scores(turn, pair):
        buf = turn % 3
        base = 128 * pair
        window_at = pl.multiple_of(turn % groups * LANES_STEP + base, 128)
        window = qbuf[:, pl.ds(window_at, ROWS)].T
        rows_of = lax.broadcasted_iota(jnp.int32, (ROWS, ROWS), 0)
        heads = []
        for i in range(2):
            start = HEAD_DIM * (2 * pair + i) - base
            heads.append(jnp.where((rows_of >= start) & (rows_of < start + HEAD_DIM), window, jnp.zeros((), jnp.bfloat16)))
        both = jnp.concatenate([heads[0][:, PIECE:], heads[1][:, PIECE:]], axis=1)
        upper = jnp.dot(kbuf[buf, half_keys:SEQ, base:base + ROWS], both, preferred_element_type=jnp.float32)
        for i in range(2):
            lower = jnp.dot(kbuf[buf, 0:half_keys, base:base + ROWS], heads[i], preferred_element_type=jnp.float32)
            s_a = lower[:, :PIECE] + hide[0:half_keys]
            s_b = lower[:, PIECE:]
            s_c = upper[:, i * PIECE:(i + 1) * PIECE] + hide[half_keys:SEQ]
            s_low[pair, i, :, 0:PIECE] = s_a
            s_low[pair, i, :, PIECE:ROWS] = s_b
            s_up[pair, i] = s_c
            m_a = jnp.max(s_a, axis=0, keepdims=True)
            m_b = jnp.maximum(jnp.max(s_b, axis=0, keepdims=True), jnp.max(s_c, axis=0, keepdims=True))
            s_max[pair, i] = jnp.broadcast_to(jnp.concatenate([m_a, m_b], axis=1), (8, ROWS))

    def attend(turn, pair):
        buf = turn % 2
        p_lowers, p_uppers, inverses = [], [], []
        for i in range(2):
            m_a, m_b = s_max[pair, i, 0:1, 0:PIECE], s_max[pair, i, 0:1, PIECE:ROWS]
            e_a = jnp.exp2((s_low[pair, i, :, 0:PIECE] - m_a) * scale)
            e_b = jnp.exp2((s_low[pair, i, :, PIECE:ROWS] - m_b) * scale)
            e_c = jnp.exp2((s_up[pair, i] - m_b) * scale)
            l_a = jnp.sum(e_a, axis=0, keepdims=True)
            l_b = jnp.sum(e_b, axis=0, keepdims=True) + jnp.sum(e_c, axis=0, keepdims=True)
            p_lowers.append(jnp.concatenate([e_a.astype(jnp.bfloat16), e_b.astype(jnp.bfloat16)], axis=1))
            p_uppers.append(e_c.astype(jnp.bfloat16))
            inverses.append(1.0 / jnp.concatenate([l_a, l_b], axis=1))
        top = 2 * pair * HEAD_DIM
        o_upper = jnp.dot(vbuf[buf, top:top + 2 * HEAD_DIM, half_keys:SEQ], jnp.concatenate(p_uppers, axis=1), preferred_element_type=jnp.float32)
        outs = []
        for i in range(2):
            o_lower = jnp.dot(vbuf[buf, top + i * HEAD_DIM:top + (i + 1) * HEAD_DIM, 0:half_keys], p_lowers[i], preferred_element_type=jnp.float32)
            mine = o_upper[i * HEAD_DIM:(i + 1) * HEAD_DIM, i * PIECE:(i + 1) * PIECE]
            o_t = jnp.concatenate([o_lower[:, :PIECE], o_lower[:, PIECE:] + mine], axis=1)
            outs.append((o_t * inverses[i]).astype(jnp.bfloat16))
        return outs

    def attend_group(turn, carry):
        wait_k(turn + 1)
        wait_v(turn)
        issue_k(turn + 2)
        issue_v(turn + 1)
        scores(turn, 1)
        outs = attend(turn, 0)
        scores(turn + 1, 0)
        outs += attend(turn, 1)
        lane = pl.ds(pl.multiple_of(turn % groups * LANES_STEP, 128), LANES_STEP)
        ubuf[:, lane] = jnp.concatenate(outs, axis=0).T
        return carry

    load_q.wait()
    load_x.wait()
    wait_k(0)

    def layer_step(layer, carry):
        w0, d0 = layer * per_layer, layer * f_tiles

        def q_step(step, carry):
            tiles = [q_pack * step + j for j in range(q_pack)]
            slots = [wait_w(w0 + i) for i in tiles]
            for i, slot in zip(tiles, slots):
                qbuf[:, cols_of(i)] = jnp.dot(ubuf[...], wbuf[slot], preferred_element_type=jnp.float32).astype(jnp.bfloat16)
            for i in tiles:
                issue_w(w0 + i + W_SLOTS)
            return carry

        @pl.when(layer > 0)
        def _():
            norm_rows(load_h, store_u, gain_of(ga_ref, layer), ROWS)
            lax.fori_loop(0, q_tiles // q_pack, q_step, 0)

        first = layer * groups
        scores(first, 0)
        lax.fori_loop(first, first + groups, attend_group, 0)

        def o_step(step, carry):
            tiles = [o_pack * step + j for j in range(o_pack)]
            slots = [wait_w(w0 + o_base + i) for i in tiles]
            for i, slot in zip(tiles, slots):
                proj = jnp.dot(ubuf[...], wbuf[slot], preferred_element_type=jnp.float32).astype(jnp.bfloat16)
                h_ref[:, cols_of(i)] = (h_ref[:, cols_of(i)].astype(jnp.float32) + proj.astype(jnp.float32)).astype(jnp.bfloat16)
            for i in tiles:
                issue_w(w0 + o_base + i + W_SLOTS)
            return carry

        lax.fori_loop(0, o_tiles // o_pack, o_step, 0)
        norm_rows(load_h, store_u, gain_of(gm_ref, layer), ROWS)
        acc[...] = jnp.zeros_like(acc)

        def up_tiles(f):
            s = w0 + f_base + 2 * f
            slot_g, slot_u = wait_w(s), wait_w(s + 1)
            gate = jnp.dot(ubuf[...], wbuf[slot_g], preferred_element_type=jnp.float32).astype(jnp.bfloat16)
            upper = jnp.dot(ubuf[...], wbuf[slot_u], preferred_element_type=jnp.float32).astype(jnp.bfloat16)
            act_new[...] = (jax.nn.silu(gate.astype(jnp.float32)) * upper.astype(jnp.float32)).astype(jnp.bfloat16)

        def up_done(f):
            s = w0 + f_base + 2 * f
            issue_w(s + W_SLOTS)
            issue_w(s + 1 + W_SLOTS)

        def down_tile(slot):
            acc[...] += jnp.dot(act_old[...], dbuf[slot], preferred_element_type=jnp.float32)

        up_tiles(0)
        act_old[...] = act_new[...]
        up_done(0)

        def f_step(f, carry):
            slot = wait_d(d0 + f - 1)
            up_tiles(f)
            down_tile(slot)
            act_old[...] = act_new[...]
            up_done(f)
            issue_d(d0 + f - 1 + D_SLOTS)
            return carry

        lax.fori_loop(1, f_tiles, f_step, 0)
        last = f_tiles - 1
        slot = wait_d(d0 + last)
        down_tile(slot)
        issue_d(d0 + last + D_SLOTS)
        h_ref[...] = (h_ref[...].astype(jnp.float32) + acc[...].astype(jnp.bfloat16).astype(jnp.float32)).astype(jnp.bfloat16)
        return carry

    lax.fori_loop(0, layers, layer_step, 0)
    wait_v(layers * groups)
    wait_k(layers * groups + 1)


def decoder_layers(rows_in, q_first, pos_rows, pos_all, all_k, all_vt, g_attn, w_q, w_o, g_mlp, w_gate, w_up, w_down):
    width = rows_in.shape[1]
    q_width = w_q.shape[2]
    layers = w_q.shape[0]
    return pl.pallas_call(
        layers_kernel,
        out_shape=jax.ShapeDtypeStruct((ROWS, width), jnp.bfloat16),
        in_specs=[SMEM, VMEM, ANY, ANY, ANY, VMEM, VMEM, ANY, ANY, ANY, ANY, ANY, ANY],
        out_specs=VMEM,
        scratch_shapes=[
            pltpu.VMEM((W_SLOTS, width, TILE), jnp.bfloat16),
            pltpu.VMEM((D_SLOTS, TILE, width), jnp.bfloat16),
            pltpu.VMEM((3, SEQ, LANES_STEP), jnp.bfloat16),
            pltpu.VMEM((2, LANES_STEP, SEQ), jnp.bfloat16),
            pltpu.VMEM((ROWS, q_width), jnp.bfloat16),
            pltpu.VMEM((ROWS, width), jnp.bfloat16),
            pltpu.VMEM((ROWS, width), jnp.float32),
            pltpu.VMEM((ROWS, TILE), jnp.bfloat16),
            pltpu.VMEM((ROWS, TILE), jnp.bfloat16),
            pltpu.VMEM((SEQ, PIECE), jnp.float32),
            pltpu.VMEM((2, 2, SEQ // 2, ROWS), jnp.float32),
            pltpu.VMEM((2, 2, SEQ // 2, PIECE), jnp.float32),
            pltpu.VMEM((2, 2, 8, ROWS), jnp.float32),
            pltpu.SMEM((2 * SP,), jnp.int32),
            pltpu.SemaphoreType.DMA((W_SLOTS,)),
            pltpu.SemaphoreType.DMA((D_SLOTS,)),
            pltpu.SemaphoreType.DMA((3,)),
            pltpu.SemaphoreType.DMA((2,)),
            pltpu.SemaphoreType.DMA((2,)),
        ],
        compiler_params=pltpu.CompilerParams(vmem_limit_bytes=VMEM_LIMIT),
        name='layers',
    )(pos_all, pos_rows.reshape(1, ROWS), rows_in, all_k, all_vt, g_attn, g_mlp, w_q, w_o.reshape(layers, q_width, width), w_gate, w_up, w_down, q_first)


def solution(mesh):
    row_spec = P(('dp', 'sp'), None)
    pos_spec = P(('dp', 'sp'))
    full = P()

    def local_step(rows_in, pos_rows, g_kv, w_k, w_v, g_attn, w_q, w_o, g_mlp, w_gate, w_up, w_down):
        all_k, all_vt, pos_all, q_first = gather_kv(rows_in, pos_rows, g_kv, w_k, w_v, g_attn, w_q)
        return decoder_layers(rows_in, q_first, pos_rows, pos_all, all_k, all_vt, g_attn, w_q, w_o, g_mlp, w_gate, w_up, w_down)

    return jax.shard_map(local_step, mesh=mesh, in_specs=(row_spec, pos_spec, full, full, full, full, full, full, full, full, full, full), out_specs=row_spec, check_vma=False)
```

```python
import functools

import jax
import jax.numpy as jnp
from jax import lax
from jax.experimental import pallas as pl
from jax.experimental.pallas import tpu as pltpu
from jax.sharding import PartitionSpec as P

NORM_EPS = 1e-6
LOG2_E = 1.4426950408889634
PIECE = 128
ROWS = 2 * PIECE
ZS = 4
SP = 2 * ZS
SEQ = SP * ROWS
HEAD_DIM = 96
HEADS_STEP = 4
LANES_STEP = HEADS_STEP * HEAD_DIM
TILE = 512
W_SLOTS = 7
D_SLOTS = 3
KV_COLS = 768
Q_COLS = 512
VMEM_LIMIT = 67_043_328
ANY = pl.BlockSpec(memory_space=pl.ANY)
VMEM = pl.BlockSpec(memory_space=pltpu.VMEM)
SMEM = pl.BlockSpec(memory_space=pltpu.SMEM)


def norm_rows(load, store, gain, rows):
    def block(i, carry):
        for part in range(4):
            at = pl.multiple_of(i * 64 + part * 16, 16)
            rows32 = load(at).astype(jnp.float32)
            inv_rms = lax.rsqrt(jnp.mean(rows32 * rows32, axis=-1, keepdims=True) + NORM_EPS)
            store(at, (rows32 * inv_rms * gain).astype(jnp.bfloat16))
        return carry

    lax.fori_loop(0, rows // 64, block, 0)


def remote_unit(z, step):
    flip = z // 2
    near = jnp.where(flip == 1, ZS - 1 - z, z)
    src_end, half_end = step // 2 + 1, step % 2
    src_mid = jnp.where(step < 4, 2 - 2 * (step % 2), 3)
    half_mid = jnp.where(step < 4, step // 2, step % 2)
    src = jnp.where(near == 0, src_end, src_mid)
    half = jnp.where(near == 0, half_end, half_mid)
    return jnp.where(flip == 1, ZS - 1 - src, src), half


def gather_kernel(x_ref, pos_ref, g_ref, wk_ref, wv_ref, ga_ref, wq_ref, k_out, vt_out, pos_out, q_out,
                  wk_buf, wv_buf, xbuf, ubuf, kst, vst, pbuf, wq_buf, qst,
                  w_sem, x_sem, out_sem, peer_send, peer_recv, wq_sem, qst_sem, recv, send_right, send_left, send_sib, psend, precv):
    sp = lax.axis_index('sp')
    z, core = sp // 2, sp % 2
    other = 1 - core
    sib = sp + 1 - 2 * core
    chunks = wk_buf.shape[0]
    cols = wk_buf.shape[2]

    def cols_of(n):
        return pl.ds(pl.multiple_of((core * chunks + n) * cols, 128), cols)

    barrier = pltpu.get_barrier_semaphore()
    for hop in range(1, SP):
        pl.semaphore_signal(barrier, inc=1, device_id={'sp': (sp + hop) % SP}, device_id_type=pl.DeviceIdType.MESH)

    def x_copy(half):
        return pltpu.make_async_copy(x_ref.at[pl.ds(half * PIECE, PIECE), :], xbuf.at[core, z, half], x_sem.at[half])

    def w_copy(n, which):
        src, dst = ((wk_ref, wk_buf), (wv_ref, wv_buf))[which]
        return pltpu.make_async_copy(src.at[:, cols_of(n)], dst.at[n], w_sem.at[which, n])

    for half in range(2):
        x_copy(half).start()
    for n in range(chunks):
        for which in range(2):
            w_copy(n, which).start()
    pl.semaphore_wait(barrier, SP - 1)

    def pos_send(hop):
        return pltpu.make_async_remote_copy(src_ref=pos_ref, dst_ref=pbuf.at[sp], send_sem=psend.at[hop], recv_sem=precv.at[sp],
                                            device_id={'sp': (sp + hop) % SP}, device_id_type=pl.DeviceIdType.MESH)

    def x_send(lane, src, half, sems, target):
        return pltpu.make_async_remote_copy(src_ref=xbuf.at[lane, src, half], dst_ref=xbuf.at[lane, src, half],
                                            send_sem=sems.at[src, half], recv_sem=recv.at[lane, src, half],
                                            device_id={'sp': target}, device_id_type=pl.DeviceIdType.MESH)

    def goes_right(src):
        return (src <= z) & (z < ZS - 1)

    def goes_left(src):
        return (src >= z) & (z > 0)

    def pass_on(src, half):
        @pl.when(goes_right(src))
        def _():
            x_send(core, src, half, send_right, sp + 2).start()

        @pl.when(goes_left(src))
        def _():
            x_send(core, src, half, send_left, sp - 2).start()

        x_send(core, src, half, send_sib, sib).start()

    for half in range(2):
        x_copy(half).wait()
        pass_on(z, half)
    for hop in range(1, SP):
        pos_send(hop).start()

    gain = g_ref[...].astype(jnp.float32).reshape(1, -1)

    def arrive(step):
        src, half = remote_unit(z, step)
        x_send(core, src, half, send_sib, sib).wait_recv()
        pass_on(src, half)

    middle = (z > 0) & (z < ZS - 1)

    def out_copies(par, unit, n, src, half):
        mine, theirs = [], []
        for lane in range(2):
            slot = (2 * src + lane) * 2 + half
            rows = pl.ds(lane * PIECE, PIECE)
            pairs = ((kst.at[par, rows, :], k_out.at[slot, :, cols_of(n)]),
                     (vst.at[par, :, rows], vt_out.at[cols_of(n), pl.ds(pl.multiple_of(slot * PIECE, PIECE), PIECE)]))
            for which, (source, target) in enumerate(pairs):
                j = 2 * lane + which
                mine.append(pltpu.make_async_copy(source, target, out_sem.at[par, j]))
                theirs.append(pltpu.make_async_remote_copy(src_ref=source, dst_ref=target, send_sem=peer_send.at[par, j], recv_sem=peer_recv.at[unit, n, j],
                                                           device_id={'sp': sib}, device_id_type=pl.DeviceIdType.MESH))
        return mine, theirs

    def out_start(par, unit, n, src, half):
        mine, theirs = out_copies(par, unit, n, src, half)
        for copy in theirs + mine:
            copy.start()

    def out_wait(par):
        mine, theirs = out_copies(par, 0, 0, 0, 0)
        for copy in mine:
            copy.wait()
        for copy in theirs:
            copy.wait_send()

    def unit_step(unit, carry):
        @pl.when(middle & ((unit == 2) | (unit == 4)))
        def _():
            arrive(unit - 2)
            arrive(unit - 1)

        @pl.when((middle & (unit >= 6)) | (jnp.logical_not(middle) & (unit >= 2)))
        def _():
            arrive(unit - 2)

        far_src, far_half = remote_unit(z, jnp.maximum(unit - 2, 0))
        src = jnp.where(unit < 2, z, far_src)
        half = jnp.where(unit < 2, unit, far_half)
        x_send(other, src, half, send_sib, sib).wait_recv()
        for lane in range(2):
            def load(at, lane=lane):
                return xbuf[lane, src, half, pl.ds(at, 16), :]

            def store(at, value, lane=lane):
                ubuf[pl.ds(lane * PIECE + at, 16), :] = value

            norm_rows(load, store, gain, PIECE)

        def chunk_step(n, carry):
            par = (unit * chunks + n) % 2

            @pl.when(unit == 0)
            def _():
                w_copy(n, 0).wait()
                w_copy(n, 1).wait()

            @pl.when(unit * chunks + n >= 2)
            def _():
                out_wait(par)

            keys = jnp.dot(ubuf[...], wk_buf[n], preferred_element_type=jnp.float32).astype(jnp.bfloat16)
            kst[par] = keys
            values = jnp.dot(ubuf[...], wv_buf[n], preferred_element_type=jnp.float32).astype(jnp.bfloat16)
            vst[par] = values.T
            out_start(par, unit, n, src, half)
            return carry

        lax.fori_loop(0, chunks, chunk_step, 0)

        return carry

    def q_copy(i):
        return pltpu.make_async_copy(wq_ref.at[0, :, pl.ds(pl.multiple_of(i * Q_COLS, 128), Q_COLS)], wq_buf.at[i % 2], wq_sem.at[i % 2])

    def q_store(i):
        return pltpu.make_async_copy(qst.at[i % 2], q_out.at[:, pl.ds(pl.multiple_of(i * Q_COLS, 128), Q_COLS)], qst_sem.at[i % 2])

    q_steps = q_out.shape[1] // Q_COLS

    def q_step(i, carry):
        q_copy(i).wait()

        @pl.when(i >= 2)
        def _():
            q_store(i).wait()

        qst[i % 2] = jnp.dot(ubuf[...], wq_buf[i % 2], preferred_element_type=jnp.float32).astype(jnp.bfloat16)
        q_store(i).start()

        @pl.when(i + 2 < q_steps)
        def _():
            q_copy(i + 2).start()

        return carry

    for i in range(2):
        q_copy(i).start()
    lax.fori_loop(0, 2, unit_step, 0)
    gain_q = ga_ref[...].astype(jnp.float32)[0:1]
    for half in range(2):
        def load(at, half=half):
            return xbuf[core, z, half, pl.ds(at, 16), :]

        def store(at, value, half=half):
            ubuf[pl.ds(half * PIECE + at, 16), :] = value

        norm_rows(load, store, gain_q, PIECE)
    lax.fori_loop(0, q_steps, q_step, 0)
    lax.fori_loop(2, 8, unit_step, 0)

    for i in range(2):
        q_store(i).wait()
    for par in range(2):
        out_wait(par)

    def peer_wait(unit, carry):
        for n in range(chunks):
            for copy in out_copies(0, unit, n, 0, 0)[1]:
                copy.wait_recv()
        return carry

    lax.fori_loop(0, 8, peer_wait, 0)

    for hop in range(1, SP):
        pos_send(hop).wait_send()
        src = (sp + hop) % SP
        pltpu.make_async_remote_copy(src_ref=pos_ref, dst_ref=pbuf.at[src], send_sem=psend.at[hop], recv_sem=precv.at[src],
                                     device_id={'sp': src}, device_id_type=pl.DeviceIdType.MESH).wait_recv()
    pbuf[sp] = pos_ref[...]
    pos_out[...] = pbuf[...]
    for src in range(ZS):
        for half in range(2):
            @pl.when(goes_right(src))
            def _(src=src, half=half):
                x_send(core, src, half, send_right, sp + 2).wait_send()

            @pl.when(goes_left(src))
            def _(src=src, half=half):
                x_send(core, src, half, send_left, sp - 2).wait_send()

            x_send(core, src, half, send_sib, sib).wait_send()


def gather_kv(rows_in, pos_rows, g_kv, w_k, w_v, g_attn, w_q):
    width = rows_in.shape[1]
    out_width = w_k.shape[1]
    cols = min(KV_COLS, out_width)
    chunks = out_width // cols // 2
    pos_tile = pos_rows.reshape(2, PIECE)
    return pl.pallas_call(
        gather_kernel,
        out_shape=(jax.ShapeDtypeStruct((2 * SP, PIECE, out_width), jnp.bfloat16),
                   jax.ShapeDtypeStruct((out_width, SEQ), jnp.bfloat16),
                   jax.ShapeDtypeStruct((SP, 2, PIECE), jnp.int32),
                   jax.ShapeDtypeStruct((ROWS, w_q.shape[2]), jnp.bfloat16)),
        in_specs=[ANY, VMEM, VMEM, ANY, ANY, VMEM, ANY],
        out_specs=(ANY, ANY, VMEM, ANY),
        scratch_shapes=[
            pltpu.VMEM((chunks, width, cols), jnp.bfloat16),
            pltpu.VMEM((chunks, width, cols), jnp.bfloat16),
            pltpu.VMEM((2, ZS, 2, PIECE, width), jnp.bfloat16),
            pltpu.VMEM((ROWS, width), jnp.bfloat16),
            pltpu.VMEM((2, ROWS, cols), jnp.bfloat16),
            pltpu.VMEM((2, cols, ROWS), jnp.bfloat16),
            pltpu.VMEM((SP, 2, PIECE), jnp.int32),
            pltpu.VMEM((2, width, Q_COLS), jnp.bfloat16),
            pltpu.VMEM((2, ROWS, Q_COLS), jnp.bfloat16),
            pltpu.SemaphoreType.DMA((2, chunks)),
            pltpu.SemaphoreType.DMA((2,)),
            pltpu.SemaphoreType.DMA((2, 4)),
            pltpu.SemaphoreType.DMA((2, 4)),
            pltpu.SemaphoreType.DMA((8, chunks, 4)),
            pltpu.SemaphoreType.DMA((2,)),
            pltpu.SemaphoreType.DMA((2,)),
            pltpu.SemaphoreType.DMA((2, ZS, 2)),
            pltpu.SemaphoreType.DMA((ZS, 2)),
            pltpu.SemaphoreType.DMA((ZS, 2)),
            pltpu.SemaphoreType.DMA((ZS, 2)),
            pltpu.SemaphoreType.DMA((SP,)),
            pltpu.SemaphoreType.DMA((SP,)),
        ],
        compiler_params=pltpu.CompilerParams(collective_id=0, has_side_effects=True, vmem_limit_bytes=VMEM_LIMIT),
        name='gather_kv',
    )(rows_in, pos_tile, g_kv, w_k, w_v, g_attn, w_q)


def layers_kernel(pos_all, qpos_ref, x_ref, k_ref, vt_ref, ga_ref, gm_ref, wq_ref, wo_ref, wg_ref, wu_ref, wd_ref, q0_ref, h_ref,
                  wbuf, dbuf, kbuf, vbuf, qbuf, ubuf, acc, act_new, act_old, hide, s_low, s_up, s_max, where_piece, w_sem, d_sem, k_sem, v_sem, h_sem):
    layers, width, q_width = wq_ref.shape
    ff = wg_ref.shape[2]
    q_tiles, o_tiles, f_tiles = q_width // TILE, width // TILE, ff // TILE
    groups = q_width // LANES_STEP
    o_base = q_tiles
    q_pack, o_pack = 2 - q_tiles % 2, 2 - o_tiles % 2
    f_base = q_tiles + o_tiles
    per_layer = f_base + 2 * f_tiles
    w_first, w_total, d_total = q_tiles, layers * per_layer, layers * f_tiles
    scale = HEAD_DIM ** -0.5 * LOG2_E

    for slot in range(2 * SP):
        where_piece[pos_all[slot // 2, slot % 2, 0] // PIECE] = slot

    def w_src(layer, ref, tile):
        return ref.at[layer, :, pl.ds(pl.multiple_of(tile * TILE, TILE), TILE)]

    def issue_w(s):
        layer, r = s // per_layer, s % per_layer
        slot = s % W_SLOTS

        def go(ref, tile):
            pltpu.make_async_copy(w_src(layer, ref, tile), wbuf.at[slot], w_sem.at[slot]).start(priority=1)

        pl.when((s < w_total) & (r < o_base))(lambda: go(wq_ref, r))
        pl.when((s < w_total) & (r >= o_base) & (r < f_base))(lambda: go(wo_ref, r - o_base))
        rr = r - f_base
        pl.when((s < w_total) & (r >= f_base) & (rr % 2 == 0))(lambda: go(wg_ref, rr // 2))
        pl.when((s < w_total) & (r >= f_base) & (rr % 2 == 1))(lambda: go(wu_ref, rr // 2))

    def wait_w(s):
        slot = s % W_SLOTS
        pltpu.make_async_copy(w_src(0, wq_ref, 0), wbuf.at[slot], w_sem.at[slot]).wait()
        return slot

    def issue_d(s):
        layer, tile = s // f_tiles, s % f_tiles
        slot = s % D_SLOTS

        @pl.when(s < d_total)
        def _():
            pltpu.make_async_copy(wd_ref.at[layer, pl.ds(pl.multiple_of(tile * TILE, TILE), TILE), :], dbuf.at[slot], d_sem.at[slot]).start(priority=1)

    def wait_d(s):
        slot = s % D_SLOTS
        pltpu.make_async_copy(wd_ref.at[0, pl.ds(0, TILE), :], dbuf.at[slot], d_sem.at[slot]).wait()
        return slot

    def issue_k(turn):
        lane = pl.multiple_of(turn % groups * LANES_STEP, 128)
        buf = turn % 3
        for piece in range(2 * SP):
            pltpu.make_async_copy(k_ref.at[where_piece[piece], :, pl.ds(lane, LANES_STEP)], kbuf.at[buf, pl.ds(piece * PIECE, PIECE), :], k_sem.at[buf]).start()

    def issue_v(turn):
        lane = pl.multiple_of(turn % groups * LANES_STEP, 128)
        buf = turn % 2
        for piece in range(2 * SP):
            col = pl.multiple_of(where_piece[piece] * PIECE, PIECE)
            pltpu.make_async_copy(vt_ref.at[pl.ds(lane, LANES_STEP), pl.ds(col, PIECE)], vbuf.at[buf, :, pl.ds(piece * PIECE, PIECE)], v_sem.at[buf]).start()

    def wait_k(turn):
        buf = turn % 3
        pltpu.make_async_copy(kbuf.at[buf], kbuf.at[buf], k_sem.at[buf]).wait()

    def wait_v(turn):
        buf = turn % 2
        pltpu.make_async_copy(vbuf.at[buf], vbuf.at[buf], v_sem.at[buf]).wait()

    issue_k(0)
    issue_v(0)
    issue_k(1)
    for s in range(w_first, w_first + W_SLOTS):
        issue_w(s)
    for s in range(D_SLOTS):
        issue_d(s)
    load_q = pltpu.make_async_copy(q0_ref, qbuf, h_sem.at[0])
    load_x = pltpu.make_async_copy(x_ref, h_ref, h_sem.at[1])
    load_q.start()
    load_x.start()

    def load_h(at):
        return h_ref[pl.ds(at, 16), :]

    def store_u(at, value):
        ubuf[pl.ds(at, 16), :] = value

    def gain_of(ref, layer):
        gains = ref[...].astype(jnp.float32)
        gain = gains[0:1]
        for other in range(1, layers):
            gain = jnp.where(layer == other, gains[other:other + 1], gain)
        return gain

    def cols_of(i):
        return pl.ds(pl.multiple_of(i * TILE, TILE), TILE)

    half_keys = SEQ // 2
    key_pos = lax.broadcasted_iota(jnp.int32, (half_keys, PIECE), 0)
    hide[0:half_keys] = jnp.where(key_pos <= qpos_ref[:, 0:PIECE], 0.0, -jnp.inf)
    hide[half_keys:SEQ] = jnp.where(key_pos + half_keys <= qpos_ref[:, PIECE:ROWS], 0.0, -jnp.inf)

    def scores(turn, pair):
        buf = turn % 3
        base = 128 * pair
        window_at = pl.multiple_of(turn % groups * LANES_STEP + base, 128)
        window = qbuf[:, pl.ds(window_at, ROWS)].T
        rows_of = lax.broadcasted_iota(jnp.int32, (ROWS, ROWS), 0)
        heads = []
        for i in range(2):
            start = HEAD_DIM * (2 * pair + i) - base
            heads.append(jnp.where((rows_of >= start) & (rows_of < start + HEAD_DIM), window, jnp.zeros((), jnp.bfloat16)))
        both = jnp.concatenate([heads[0][:, PIECE:], heads[1][:, PIECE:]], axis=1)
        upper = jnp.dot(kbuf[buf, half_keys:SEQ, base:base + ROWS], both, preferred_element_type=jnp.float32)
        for i in range(2):
            lower = jnp.dot(kbuf[buf, 0:half_keys, base:base + ROWS], heads[i], preferred_element_type=jnp.float32)
            s_a = lower[:, :PIECE] + hide[0:half_keys]
            s_b = lower[:, PIECE:]
            s_c = upper[:, i * PIECE:(i + 1) * PIECE] + hide[half_keys:SEQ]
            s_low[pair, i, :, 0:PIECE] = s_a
            s_low[pair, i, :, PIECE:ROWS] = s_b
            s_up[pair, i] = s_c
            m_a = jnp.max(s_a, axis=0, keepdims=True)
            m_b = jnp.maximum(jnp.max(s_b, axis=0, keepdims=True), jnp.max(s_c, axis=0, keepdims=True))
            s_max[pair, i] = jnp.broadcast_to(jnp.concatenate([m_a, m_b], axis=1), (8, ROWS))

    def attend(turn, pair):
        buf = turn % 2
        p_lowers, p_uppers, inverses = [], [], []
        for i in range(2):
            m_a, m_b = s_max[pair, i, 0:1, 0:PIECE], s_max[pair, i, 0:1, PIECE:ROWS]
            e_a = jnp.exp2((s_low[pair, i, :, 0:PIECE] - m_a) * scale)
            e_b = jnp.exp2((s_low[pair, i, :, PIECE:ROWS] - m_b) * scale)
            e_c = jnp.exp2((s_up[pair, i] - m_b) * scale)
            l_a = jnp.sum(e_a, axis=0, keepdims=True)
            l_b = jnp.sum(e_b, axis=0, keepdims=True) + jnp.sum(e_c, axis=0, keepdims=True)
            p_lowers.append(jnp.concatenate([e_a.astype(jnp.bfloat16), e_b.astype(jnp.bfloat16)], axis=1))
            p_uppers.append(e_c.astype(jnp.bfloat16))
            inverses.append(1.0 / jnp.concatenate([l_a, l_b], axis=1))
        top = 2 * pair * HEAD_DIM
        o_upper = jnp.dot(vbuf[buf, top:top + 2 * HEAD_DIM, half_keys:SEQ], jnp.concatenate(p_uppers, axis=1), preferred_element_type=jnp.float32)
        outs = []
        for i in range(2):
            o_lower = jnp.dot(vbuf[buf, top + i * HEAD_DIM:top + (i + 1) * HEAD_DIM, 0:half_keys], p_lowers[i], preferred_element_type=jnp.float32)
            mine = o_upper[i * HEAD_DIM:(i + 1) * HEAD_DIM, i * PIECE:(i + 1) * PIECE]
            o_t = jnp.concatenate([o_lower[:, :PIECE], o_lower[:, PIECE:] + mine], axis=1)
            outs.append((o_t * inverses[i]).astype(jnp.bfloat16))
        return outs

    def attend_group(turn, carry):
        wait_k(turn + 1)
        wait_v(turn)
        issue_k(turn + 2)
        issue_v(turn + 1)
        scores(turn, 1)
        outs = attend(turn, 0)
        scores(turn + 1, 0)
        outs += attend(turn, 1)
        lane = pl.ds(pl.multiple_of(turn % groups * LANES_STEP, 128), LANES_STEP)
        ubuf[:, lane] = jnp.concatenate(outs, axis=0).T
        return carry

    load_q.wait()
    load_x.wait()
    wait_k(0)

    def layer_step(layer, carry):
        w0, d0 = layer * per_layer, layer * f_tiles

        def q_step(step, carry):
            tiles = [q_pack * step + j for j in range(q_pack)]
            slots = [wait_w(w0 + i) for i in tiles]
            for i, slot in zip(tiles, slots):
                qbuf[:, cols_of(i)] = jnp.dot(ubuf[...], wbuf[slot], preferred_element_type=jnp.float32).astype(jnp.bfloat16)
            for i in tiles:
                issue_w(w0 + i + W_SLOTS)
            return carry

        @pl.when(layer > 0)
        def _():
            norm_rows(load_h, store_u, gain_of(ga_ref, layer), ROWS)
            lax.fori_loop(0, q_tiles // q_pack, q_step, 0)

        first = layer * groups
        scores(first, 0)
        lax.fori_loop(first, first + groups, attend_group, 0)

        def o_step(step, carry):
            tiles = [o_pack * step + j for j in range(o_pack)]
            slots = [wait_w(w0 + o_base + i) for i in tiles]
            for i, slot in zip(tiles, slots):
                proj = jnp.dot(ubuf[...], wbuf[slot], preferred_element_type=jnp.float32).astype(jnp.bfloat16)
                h_ref[:, cols_of(i)] = (h_ref[:, cols_of(i)].astype(jnp.float32) + proj.astype(jnp.float32)).astype(jnp.bfloat16)
            for i in tiles:
                issue_w(w0 + o_base + i + W_SLOTS)
            return carry

        lax.fori_loop(0, o_tiles // o_pack, o_step, 0)
        norm_rows(load_h, store_u, gain_of(gm_ref, layer), ROWS)
        acc[...] = jnp.zeros_like(acc)

        def up_tiles(f):
            s = w0 + f_base + 2 * f
            slot_g, slot_u = wait_w(s), wait_w(s + 1)
            gate = jnp.dot(ubuf[...], wbuf[slot_g], preferred_element_type=jnp.float32).astype(jnp.bfloat16)
            upper = jnp.dot(ubuf[...], wbuf[slot_u], preferred_element_type=jnp.float32).astype(jnp.bfloat16)
            act_new[...] = (jax.nn.silu(gate.astype(jnp.float32)) * upper.astype(jnp.float32)).astype(jnp.bfloat16)

        def up_done(f):
            s = w0 + f_base + 2 * f
            issue_w(s + W_SLOTS)
            issue_w(s + 1 + W_SLOTS)

        def down_tile(slot):
            acc[...] += jnp.dot(act_old[...], dbuf[slot], preferred_element_type=jnp.float32)

        up_tiles(0)
        act_old[...] = act_new[...]
        up_done(0)

        def f_step(f, carry):
            slot = wait_d(d0 + f - 1)
            up_tiles(f)
            down_tile(slot)
            act_old[...] = act_new[...]
            up_done(f)
            issue_d(d0 + f - 1 + D_SLOTS)
            return carry

        lax.fori_loop(1, f_tiles, f_step, 0)
        last = f_tiles - 1
        slot = wait_d(d0 + last)
        down_tile(slot)
        issue_d(d0 + last + D_SLOTS)
        h_ref[...] = (h_ref[...].astype(jnp.float32) + acc[...].astype(jnp.bfloat16).astype(jnp.float32)).astype(jnp.bfloat16)
        return carry

    lax.fori_loop(0, layers, layer_step, 0)
    wait_v(layers * groups)
    wait_k(layers * groups + 1)


def decoder_layers(rows_in, q_first, pos_rows, pos_all, all_k, all_vt, g_attn, w_q, w_o, g_mlp, w_gate, w_up, w_down):
    width = rows_in.shape[1]
    q_width = w_q.shape[2]
    layers = w_q.shape[0]
    return pl.pallas_call(
        layers_kernel,
        out_shape=jax.ShapeDtypeStruct((ROWS, width), jnp.bfloat16),
        in_specs=[SMEM, VMEM, ANY, ANY, ANY, VMEM, VMEM, ANY, ANY, ANY, ANY, ANY, ANY],
        out_specs=VMEM,
        scratch_shapes=[
            pltpu.VMEM((W_SLOTS, width, TILE), jnp.bfloat16),
            pltpu.VMEM((D_SLOTS, TILE, width), jnp.bfloat16),
            pltpu.VMEM((3, SEQ, LANES_STEP), jnp.bfloat16),
            pltpu.VMEM((2, LANES_STEP, SEQ), jnp.bfloat16),
            pltpu.VMEM((ROWS, q_width), jnp.bfloat16),
            pltpu.VMEM((ROWS, width), jnp.bfloat16),
            pltpu.VMEM((ROWS, width), jnp.float32),
            pltpu.VMEM((ROWS, TILE), jnp.bfloat16),
            pltpu.VMEM((ROWS, TILE), jnp.bfloat16),
            pltpu.VMEM((SEQ, PIECE), jnp.float32),
            pltpu.VMEM((2, 2, SEQ // 2, ROWS), jnp.float32),
            pltpu.VMEM((2, 2, SEQ // 2, PIECE), jnp.float32),
            pltpu.VMEM((2, 2, 8, ROWS), jnp.float32),
            pltpu.SMEM((2 * SP,), jnp.int32),
            pltpu.SemaphoreType.DMA((W_SLOTS,)),
            pltpu.SemaphoreType.DMA((D_SLOTS,)),
            pltpu.SemaphoreType.DMA((3,)),
            pltpu.SemaphoreType.DMA((2,)),
            pltpu.SemaphoreType.DMA((2,)),
        ],
        compiler_params=pltpu.CompilerParams(vmem_limit_bytes=VMEM_LIMIT),
        name='layers',
    )(pos_all, pos_rows.reshape(1, ROWS), rows_in, all_k, all_vt, g_attn, g_mlp, w_q, w_o.reshape(layers, q_width, width), w_gate, w_up, w_down, q_first)


def solution(mesh):
    row_spec = P(('dp', 'sp'), None)
    pos_spec = P(('dp', 'sp'))
    full = P()

    def local_step(rows_in, pos_rows, g_kv, w_k, w_v, g_attn, w_q, w_o, g_mlp, w_gate, w_up, w_down):
        all_k, all_vt, pos_all, q_first = gather_kv(rows_in, pos_rows, g_kv, w_k, w_v, g_attn, w_q)
        return decoder_layers(rows_in, q_first, pos_rows, pos_all, all_k, all_vt, g_attn, w_q, w_o, g_mlp, w_gate, w_up, w_down)

    return jax.shard_map(local_step, mesh=mesh, in_specs=(row_spec, pos_spec, full, full, full, full, full, full, full, full, full, full), out_specs=row_spec, check_vma=False)
```

```python
import functools

import jax
import jax.numpy as jnp
from jax import lax
from jax.experimental import pallas as pl
from jax.experimental.pallas import tpu as pltpu
from jax.sharding import PartitionSpec as P

NORM_EPS = 1e-6
LOG2_E = 1.4426950408889634
PIECE = 128
ROWS = 2 * PIECE
ZS = 4
SP = 2 * ZS
SEQ = SP * ROWS
HEAD_DIM = 96
HEADS_STEP = 4
LANES_STEP = HEADS_STEP * HEAD_DIM
TILE = 512
W_SLOTS = 8
D_SLOTS = 3
KV_COLS = 768
Q_COLS = 512
VMEM_LIMIT = 67_043_328
ANY = pl.BlockSpec(memory_space=pl.ANY)
VMEM = pl.BlockSpec(memory_space=pltpu.VMEM)
SMEM = pl.BlockSpec(memory_space=pltpu.SMEM)


def norm_rows(load, store, gain, rows):
    def block(i, carry):
        for part in range(4):
            at = pl.multiple_of(i * 64 + part * 16, 16)
            rows32 = load(at).astype(jnp.float32)
            inv_rms = lax.rsqrt(jnp.mean(rows32 * rows32, axis=-1, keepdims=True) + NORM_EPS)
            store(at, (rows32 * inv_rms * gain).astype(jnp.bfloat16))
        return carry

    lax.fori_loop(0, rows // 64, block, 0)


def remote_unit(z, step):
    flip = z // 2
    near = jnp.where(flip == 1, ZS - 1 - z, z)
    src_end, half_end = step // 2 + 1, step % 2
    src_mid = jnp.where(step < 4, 2 - 2 * (step % 2), 3)
    half_mid = jnp.where(step < 4, step // 2, step % 2)
    src = jnp.where(near == 0, src_end, src_mid)
    half = jnp.where(near == 0, half_end, half_mid)
    return jnp.where(flip == 1, ZS - 1 - src, src), half


def gather_kernel(x_ref, pos_ref, g_ref, wk_ref, wv_ref, ga_ref, wq_ref, k_out, vt_out, pos_out, q_out,
                  wk_buf, wv_buf, xbuf, ubuf, kst, vst, pbuf, wq_buf, qst,
                  w_sem, x_sem, out_sem, peer_send, peer_recv, wq_sem, qst_sem, recv, send_right, send_left, send_sib, psend, precv):
    sp = lax.axis_index('sp')
    z, core = sp // 2, sp % 2
    other = 1 - core
    sib = sp + 1 - 2 * core
    chunks = wk_buf.shape[0]
    cols = wk_buf.shape[2]

    def cols_of(n):
        return pl.ds(pl.multiple_of((core * chunks + n) * cols, 128), cols)

    barrier = pltpu.get_barrier_semaphore()
    for hop in range(1, SP):
        pl.semaphore_signal(barrier, inc=1, device_id={'sp': (sp + hop) % SP}, device_id_type=pl.DeviceIdType.MESH)

    def x_copy(half):
        return pltpu.make_async_copy(x_ref.at[pl.ds(half * PIECE, PIECE), :], xbuf.at[core, z, half], x_sem.at[half])

    def w_copy(n, which):
        src, dst = ((wk_ref, wk_buf), (wv_ref, wv_buf))[which]
        return pltpu.make_async_copy(src.at[:, cols_of(n)], dst.at[n], w_sem.at[which, n])

    for half in range(2):
        x_copy(half).start()
    for n in range(chunks):
        for which in range(2):
            w_copy(n, which).start()
    pl.semaphore_wait(barrier, SP - 1)

    def pos_send(hop):
        return pltpu.make_async_remote_copy(src_ref=pos_ref, dst_ref=pbuf.at[sp], send_sem=psend.at[hop], recv_sem=precv.at[sp],
                                            device_id={'sp': (sp + hop) % SP}, device_id_type=pl.DeviceIdType.MESH)

    def x_send(lane, src, half, sems, target):
        return pltpu.make_async_remote_copy(src_ref=xbuf.at[lane, src, half], dst_ref=xbuf.at[lane, src, half],
                                            send_sem=sems.at[src, half], recv_sem=recv.at[lane, src, half],
                                            device_id={'sp': target}, device_id_type=pl.DeviceIdType.MESH)

    def goes_right(src):
        return (src <= z) & (z < ZS - 1)

    def goes_left(src):
        return (src >= z) & (z > 0)

    def pass_on(src, half):
        @pl.when(goes_right(src))
        def _():
            x_send(core, src, half, send_right, sp + 2).start()

        @pl.when(goes_left(src))
        def _():
            x_send(core, src, half, send_left, sp - 2).start()

        x_send(core, src, half, send_sib, sib).start()

    for half in range(2):
        x_copy(half).wait()
        pass_on(z, half)
    for hop in range(1, SP):
        pos_send(hop).start()

    gain = g_ref[...].astype(jnp.float32).reshape(1, -1)

    def arrive(step):
        src, half = remote_unit(z, step)
        x_send(core, src, half, send_sib, sib).wait_recv()
        pass_on(src, half)

    middle = (z > 0) & (z < ZS - 1)

    def out_copies(par, unit, n, src, half):
        mine, theirs = [], []
        for lane in range(2):
            slot = (2 * src + lane) * 2 + half
            rows = pl.ds(lane * PIECE, PIECE)
            pairs = ((kst.at[par, rows, :], k_out.at[slot, :, cols_of(n)]),
                     (vst.at[par, :, rows], vt_out.at[cols_of(n), pl.ds(pl.multiple_of(slot * PIECE, PIECE), PIECE)]))
            for which, (source, target) in enumerate(pairs):
                j = 2 * lane + which
                mine.append(pltpu.make_async_copy(source, target, out_sem.at[par, j]))
                theirs.append(pltpu.make_async_remote_copy(src_ref=source, dst_ref=target, send_sem=peer_send.at[par, j], recv_sem=peer_recv.at[unit, n, j],
                                                           device_id={'sp': sib}, device_id_type=pl.DeviceIdType.MESH))
        return mine, theirs

    def out_start(par, unit, n, src, half):
        mine, theirs = out_copies(par, unit, n, src, half)
        for copy in theirs + mine:
            copy.start()

    def out_wait(par):
        mine, theirs = out_copies(par, 0, 0, 0, 0)
        for copy in mine:
            copy.wait()
        for copy in theirs:
            copy.wait_send()

    def unit_step(unit, carry):
        @pl.when(middle & ((unit == 2) | (unit == 4)))
        def _():
            arrive(unit - 2)
            arrive(unit - 1)

        @pl.when((middle & (unit >= 6)) | (jnp.logical_not(middle) & (unit >= 2)))
        def _():
            arrive(unit - 2)

        far_src, far_half = remote_unit(z, jnp.maximum(unit - 2, 0))
        src = jnp.where(unit < 2, z, far_src)
        half = jnp.where(unit < 2, unit, far_half)

        def normalise(lane):
            def load(at):
                return xbuf[lane, src, half, pl.ds(at, 16), :]

            def store(at, value):
                ubuf[pl.ds(pl.multiple_of(lane * PIECE + at, 16), 16), :] = value

            norm_rows(load, store, gain, PIECE)

        normalise(core)
        x_send(other, src, half, send_sib, sib).wait_recv()
        normalise(other)

        def chunk_step(n, carry):
            par = (unit * chunks + n) % 2

            @pl.when(unit == 0)
            def _():
                w_copy(n, 0).wait()
                w_copy(n, 1).wait()

            @pl.when(unit * chunks + n >= 2)
            def _():
                out_wait(par)

            keys = jnp.dot(ubuf[...], wk_buf[n], preferred_element_type=jnp.float32).astype(jnp.bfloat16)
            kst[par] = keys
            values = jnp.dot(ubuf[...], wv_buf[n], preferred_element_type=jnp.float32).astype(jnp.bfloat16)
            vst[par] = values.T
            out_start(par, unit, n, src, half)
            return carry

        lax.fori_loop(0, chunks, chunk_step, 0)

        return carry

    def q_copy(i):
        return pltpu.make_async_copy(wq_ref.at[0, :, pl.ds(pl.multiple_of(i * Q_COLS, 128), Q_COLS)], wq_buf.at[i % 2], wq_sem.at[i % 2])

    def q_store(i):
        return pltpu.make_async_copy(qst.at[i % 2], q_out.at[:, pl.ds(pl.multiple_of(i * Q_COLS, 128), Q_COLS)], qst_sem.at[i % 2])

    q_steps = q_out.shape[1] // Q_COLS

    def q_step(i, carry):
        q_copy(i).wait()

        @pl.when(i >= 2)
        def _():
            q_store(i).wait()

        qst[i % 2] = jnp.dot(ubuf[...], wq_buf[i % 2], preferred_element_type=jnp.float32).astype(jnp.bfloat16)
        q_store(i).start()

        @pl.when(i + 2 < q_steps)
        def _():
            q_copy(i + 2).start()

        return carry

    for i in range(2):
        q_copy(i).start()
    lax.fori_loop(0, 2, unit_step, 0)
    gain_q = ga_ref[...].astype(jnp.float32)[0:1]
    for half in range(2):
        def load(at, half=half):
            return xbuf[core, z, half, pl.ds(at, 16), :]

        def store(at, value, half=half):
            ubuf[pl.ds(half * PIECE + at, 16), :] = value

        norm_rows(load, store, gain_q, PIECE)
    lax.fori_loop(0, q_steps, q_step, 0)
    lax.fori_loop(2, 8, unit_step, 0)

    for i in range(2):
        q_store(i).wait()
    for par in range(2):
        out_wait(par)

    def peer_wait(unit, carry):
        for n in range(chunks):
            for copy in out_copies(0, unit, n, 0, 0)[1]:
                copy.wait_recv()
        return carry

    lax.fori_loop(0, 8, peer_wait, 0)

    for hop in range(1, SP):
        pos_send(hop).wait_send()
        src = (sp + hop) % SP
        pltpu.make_async_remote_copy(src_ref=pos_ref, dst_ref=pbuf.at[src], send_sem=psend.at[hop], recv_sem=precv.at[src],
                                     device_id={'sp': src}, device_id_type=pl.DeviceIdType.MESH).wait_recv()
    pbuf[sp] = pos_ref[...]
    pos_out[...] = pbuf[...]
    for src in range(ZS):
        for half in range(2):
            @pl.when(goes_right(src))
            def _(src=src, half=half):
                x_send(core, src, half, send_right, sp + 2).wait_send()

            @pl.when(goes_left(src))
            def _(src=src, half=half):
                x_send(core, src, half, send_left, sp - 2).wait_send()

            x_send(core, src, half, send_sib, sib).wait_send()


def gather_kv(rows_in, pos_rows, g_kv, w_k, w_v, g_attn, w_q):
    width = rows_in.shape[1]
    out_width = w_k.shape[1]
    cols = min(KV_COLS, out_width)
    chunks = out_width // cols // 2
    pos_tile = pos_rows.reshape(2, PIECE)
    return pl.pallas_call(
        gather_kernel,
        out_shape=(jax.ShapeDtypeStruct((2 * SP, PIECE, out_width), jnp.bfloat16),
                   jax.ShapeDtypeStruct((out_width, SEQ), jnp.bfloat16),
                   jax.ShapeDtypeStruct((SP, 2, PIECE), jnp.int32),
                   jax.ShapeDtypeStruct((ROWS, w_q.shape[2]), jnp.bfloat16)),
        in_specs=[ANY, VMEM, VMEM, ANY, ANY, VMEM, ANY],
        out_specs=(ANY, ANY, VMEM, ANY),
        scratch_shapes=[
            pltpu.VMEM((chunks, width, cols), jnp.bfloat16),
            pltpu.VMEM((chunks, width, cols), jnp.bfloat16),
            pltpu.VMEM((2, ZS, 2, PIECE, width), jnp.bfloat16),
            pltpu.VMEM((ROWS, width), jnp.bfloat16),
            pltpu.VMEM((2, ROWS, cols), jnp.bfloat16),
            pltpu.VMEM((2, cols, ROWS), jnp.bfloat16),
            pltpu.VMEM((SP, 2, PIECE), jnp.int32),
            pltpu.VMEM((2, width, Q_COLS), jnp.bfloat16),
            pltpu.VMEM((2, ROWS, Q_COLS), jnp.bfloat16),
            pltpu.SemaphoreType.DMA((2, chunks)),
            pltpu.SemaphoreType.DMA((2,)),
            pltpu.SemaphoreType.DMA((2, 4)),
            pltpu.SemaphoreType.DMA((2, 4)),
            pltpu.SemaphoreType.DMA((8, chunks, 4)),
            pltpu.SemaphoreType.DMA((2,)),
            pltpu.SemaphoreType.DMA((2,)),
            pltpu.SemaphoreType.DMA((2, ZS, 2)),
            pltpu.SemaphoreType.DMA((ZS, 2)),
            pltpu.SemaphoreType.DMA((ZS, 2)),
            pltpu.SemaphoreType.DMA((ZS, 2)),
            pltpu.SemaphoreType.DMA((SP,)),
            pltpu.SemaphoreType.DMA((SP,)),
        ],
        compiler_params=pltpu.CompilerParams(collective_id=0, has_side_effects=True, vmem_limit_bytes=VMEM_LIMIT),
        name='gather_kv',
    )(rows_in, pos_tile, g_kv, w_k, w_v, g_attn, w_q)


def layers_kernel(pos_all, qpos_ref, x_ref, k_ref, vt_ref, ga_ref, gm_ref, wq_ref, wo_ref, wg_ref, wu_ref, wd_ref, q0_ref, h_ref,
                  wbuf, dbuf, kbuf, vbuf, qbuf, ubuf, acc, act_new, act_old, hide, s_low, s_up, s_max, where_piece, w_sem, d_sem, k_sem, v_sem, h_sem):
    layers, width, q_width = wq_ref.shape
    ff = wg_ref.shape[2]
    q_tiles, o_tiles, f_tiles = q_width // TILE, width // TILE, ff // TILE
    groups = q_width // LANES_STEP
    o_base = q_tiles
    q_pack, o_pack = 2 - q_tiles % 2, 2 - o_tiles % 2
    f_base = q_tiles + o_tiles
    per_layer = f_base + 2 * f_tiles
    w_first, w_total, d_total = q_tiles, layers * per_layer, layers * f_tiles
    scale = HEAD_DIM ** -0.5 * LOG2_E

    for slot in range(2 * SP):
        where_piece[pos_all[slot // 2, slot % 2, 0] // PIECE] = slot

    def w_src(layer, ref, tile):
        return ref.at[layer, :, pl.ds(pl.multiple_of(tile * TILE, TILE), TILE)]

    def issue_w(s):
        layer, r = s // per_layer, s % per_layer
        slot = s % W_SLOTS

        def go(ref, tile):
            pltpu.make_async_copy(w_src(layer, ref, tile), wbuf.at[slot], w_sem.at[slot]).start(priority=1)

        pl.when((s < w_total) & (r < o_base))(lambda: go(wq_ref, r))
        pl.when((s < w_total) & (r >= o_base) & (r < f_base))(lambda: go(wo_ref, r - o_base))
        rr = r - f_base
        pl.when((s < w_total) & (r >= f_base) & (rr % 2 == 0))(lambda: go(wg_ref, rr // 2))
        pl.when((s < w_total) & (r >= f_base) & (rr % 2 == 1))(lambda: go(wu_ref, rr // 2))

    def wait_w(s):
        slot = s % W_SLOTS
        pltpu.make_async_copy(w_src(0, wq_ref, 0), wbuf.at[slot], w_sem.at[slot]).wait()
        return slot

    def issue_d(s):
        layer, tile = s // f_tiles, s % f_tiles
        slot = s % D_SLOTS

        @pl.when(s < d_total)
        def _():
            pltpu.make_async_copy(wd_ref.at[layer, pl.ds(pl.multiple_of(tile * TILE, TILE), TILE), :], dbuf.at[slot], d_sem.at[slot]).start(priority=1)

    def wait_d(s):
        slot = s % D_SLOTS
        pltpu.make_async_copy(wd_ref.at[0, pl.ds(0, TILE), :], dbuf.at[slot], d_sem.at[slot]).wait()
        return slot

    def issue_k(turn):
        lane = pl.multiple_of(turn % groups * LANES_STEP, 128)
        buf = turn % 3
        for piece in range(2 * SP):
            pltpu.make_async_copy(k_ref.at[where_piece[piece], :, pl.ds(lane, LANES_STEP)], kbuf.at[buf, pl.ds(piece * PIECE, PIECE), :], k_sem.at[buf]).start()

    def issue_v(turn):
        lane = pl.multiple_of(turn % groups * LANES_STEP, 128)
        buf = turn % 2
        for piece in range(2 * SP):
            col = pl.multiple_of(where_piece[piece] * PIECE, PIECE)
            pltpu.make_async_copy(vt_ref.at[pl.ds(lane, LANES_STEP), pl.ds(col, PIECE)], vbuf.at[buf, :, pl.ds(piece * PIECE, PIECE)], v_sem.at[buf]).start()

    def wait_k(turn):
        buf = turn % 3
        pltpu.make_async_copy(kbuf.at[buf], kbuf.at[buf], k_sem.at[buf]).wait()

    def wait_v(turn):
        buf = turn % 2
        pltpu.make_async_copy(vbuf.at[buf], vbuf.at[buf], v_sem.at[buf]).wait()

    issue_k(0)
    issue_v(0)
    issue_k(1)
    for s in range(w_first, w_first + W_SLOTS):
        issue_w(s)
    for s in range(D_SLOTS):
        issue_d(s)
    load_q = pltpu.make_async_copy(q0_ref, qbuf, h_sem.at[0])
    load_x = pltpu.make_async_copy(x_ref, h_ref, h_sem.at[1])
    load_q.start()
    load_x.start()

    def load_h(at):
        return h_ref[pl.ds(at, 16), :]

    def store_u(at, value):
        ubuf[pl.ds(at, 16), :] = value

    def gain_of(ref, layer):
        gains = ref[...].astype(jnp.float32)
        gain = gains[0:1]
        for other in range(1, layers):
            gain = jnp.where(layer == other, gains[other:other + 1], gain)
        return gain

    def cols_of(i):
        return pl.ds(pl.multiple_of(i * TILE, TILE), TILE)

    half_keys = SEQ // 2
    key_pos = lax.broadcasted_iota(jnp.int32, (half_keys, PIECE), 0)
    hide[0:half_keys] = jnp.where(key_pos <= qpos_ref[:, 0:PIECE], 0.0, -jnp.inf)
    hide[half_keys:SEQ] = jnp.where(key_pos + half_keys <= qpos_ref[:, PIECE:ROWS], 0.0, -jnp.inf)

    def scores(turn, pair):
        buf = turn % 3
        base = 128 * pair
        window_at = pl.multiple_of(turn % groups * LANES_STEP + base, 128)
        window = qbuf[:, pl.ds(window_at, ROWS)].T
        rows_of = lax.broadcasted_iota(jnp.int32, (ROWS, ROWS), 0)
        heads = []
        for i in range(2):
            start = HEAD_DIM * (2 * pair + i) - base
            heads.append(jnp.where((rows_of >= start) & (rows_of < start + HEAD_DIM), window, jnp.zeros((), jnp.bfloat16)))
        both = jnp.concatenate([heads[0][:, PIECE:], heads[1][:, PIECE:]], axis=1)
        upper = jnp.dot(kbuf[buf, half_keys:SEQ, base:base + ROWS], both, preferred_element_type=jnp.float32)
        for i in range(2):
            lower = jnp.dot(kbuf[buf, 0:half_keys, base:base + ROWS], heads[i], preferred_element_type=jnp.float32)
            s_a = lower[:, :PIECE] + hide[0:half_keys]
            s_b = lower[:, PIECE:]
            s_c = upper[:, i * PIECE:(i + 1) * PIECE] + hide[half_keys:SEQ]
            s_low[pair, i, :, 0:PIECE] = s_a
            s_low[pair, i, :, PIECE:ROWS] = s_b
            s_up[pair, i] = s_c
            m_a = jnp.max(s_a, axis=0, keepdims=True)
            m_b = jnp.maximum(jnp.max(s_b, axis=0, keepdims=True), jnp.max(s_c, axis=0, keepdims=True))
            s_max[pair, i] = jnp.broadcast_to(jnp.concatenate([m_a, m_b], axis=1), (8, ROWS))

    def attend(turn, pair):
        buf = turn % 2
        p_lowers, p_uppers, inverses = [], [], []
        for i in range(2):
            m_a, m_b = s_max[pair, i, 0:1, 0:PIECE], s_max[pair, i, 0:1, PIECE:ROWS]
            e_a = jnp.exp2((s_low[pair, i, :, 0:PIECE] - m_a) * scale)
            e_b = jnp.exp2((s_low[pair, i, :, PIECE:ROWS] - m_b) * scale)
            e_c = jnp.exp2((s_up[pair, i] - m_b) * scale)
            l_a = jnp.sum(e_a, axis=0, keepdims=True)
            l_b = jnp.sum(e_b, axis=0, keepdims=True) + jnp.sum(e_c, axis=0, keepdims=True)
            p_lowers.append(jnp.concatenate([e_a.astype(jnp.bfloat16), e_b.astype(jnp.bfloat16)], axis=1))
            p_uppers.append(e_c.astype(jnp.bfloat16))
            inverses.append(1.0 / jnp.concatenate([l_a, l_b], axis=1))
        top = 2 * pair * HEAD_DIM
        o_upper = jnp.dot(vbuf[buf, top:top + 2 * HEAD_DIM, half_keys:SEQ], jnp.concatenate(p_uppers, axis=1), preferred_element_type=jnp.float32)
        outs = []
        for i in range(2):
            o_lower = jnp.dot(vbuf[buf, top + i * HEAD_DIM:top + (i + 1) * HEAD_DIM, 0:half_keys], p_lowers[i], preferred_element_type=jnp.float32)
            mine = o_upper[i * HEAD_DIM:(i + 1) * HEAD_DIM, i * PIECE:(i + 1) * PIECE]
            o_t = jnp.concatenate([o_lower[:, :PIECE], o_lower[:, PIECE:] + mine], axis=1)
            outs.append((o_t * inverses[i]).astype(jnp.bfloat16))
        return outs

    def attend_group(turn, carry):
        wait_k(turn + 1)
        wait_v(turn)
        issue_k(turn + 2)
        issue_v(turn + 1)
        scores(turn, 1)
        outs = attend(turn, 0)
        scores(turn + 1, 0)
        outs += attend(turn, 1)
        lane = pl.ds(pl.multiple_of(turn % groups * LANES_STEP, 128), LANES_STEP)
        ubuf[:, lane] = jnp.concatenate(outs, axis=0).T
        return carry

    load_q.wait()
    load_x.wait()
    wait_k(0)

    def layer_step(layer, carry):
        w0, d0 = layer * per_layer, layer * f_tiles

        def q_step(step, carry):
            tiles = [q_pack * step + j for j in range(q_pack)]
            slots = [wait_w(w0 + i) for i in tiles]
            for i, slot in zip(tiles, slots):
                qbuf[:, cols_of(i)] = jnp.dot(ubuf[...], wbuf[slot], preferred_element_type=jnp.float32).astype(jnp.bfloat16)
            for i in tiles:
                issue_w(w0 + i + W_SLOTS)
            return carry

        @pl.when(layer > 0)
        def _():
            norm_rows(load_h, store_u, gain_of(ga_ref, layer), ROWS)
            lax.fori_loop(0, q_tiles // q_pack, q_step, 0)

        first = layer * groups
        scores(first, 0)
        lax.fori_loop(first, first + groups, attend_group, 0)

        def o_step(step, carry):
            tiles = [o_pack * step + j for j in range(o_pack)]
            slots = [wait_w(w0 + o_base + i) for i in tiles]
            for i, slot in zip(tiles, slots):
                proj = jnp.dot(ubuf[...], wbuf[slot], preferred_element_type=jnp.float32).astype(jnp.bfloat16)
                h_ref[:, cols_of(i)] = (h_ref[:, cols_of(i)].astype(jnp.float32) + proj.astype(jnp.float32)).astype(jnp.bfloat16)
            for i in tiles:
                issue_w(w0 + o_base + i + W_SLOTS)
            return carry

        lax.fori_loop(0, o_tiles // o_pack, o_step, 0)
        norm_rows(load_h, store_u, gain_of(gm_ref, layer), ROWS)
        acc[...] = jnp.zeros_like(acc)

        def up_tiles(f):
            s = w0 + f_base + 2 * f
            slot_g, slot_u = wait_w(s), wait_w(s + 1)
            gate = jnp.dot(ubuf[...], wbuf[slot_g], preferred_element_type=jnp.float32).astype(jnp.bfloat16)
            upper = jnp.dot(ubuf[...], wbuf[slot_u], preferred_element_type=jnp.float32).astype(jnp.bfloat16)
            act_new[...] = (jax.nn.silu(gate.astype(jnp.float32)) * upper.astype(jnp.float32)).astype(jnp.bfloat16)

        def up_done(f):
            s = w0 + f_base + 2 * f
            issue_w(s + W_SLOTS)
            issue_w(s + 1 + W_SLOTS)

        def down_tile(slot):
            acc[...] += jnp.dot(act_old[...], dbuf[slot], preferred_element_type=jnp.float32)

        up_tiles(0)
        act_old[...] = act_new[...]
        up_done(0)

        def f_step(f, carry):
            slot = wait_d(d0 + f - 1)
            up_tiles(f)
            down_tile(slot)
            act_old[...] = act_new[...]
            up_done(f)
            issue_d(d0 + f - 1 + D_SLOTS)
            return carry

        lax.fori_loop(1, f_tiles, f_step, 0)
        last = f_tiles - 1
        slot = wait_d(d0 + last)
        down_tile(slot)
        issue_d(d0 + last + D_SLOTS)
        h_ref[...] = (h_ref[...].astype(jnp.float32) + acc[...].astype(jnp.bfloat16).astype(jnp.float32)).astype(jnp.bfloat16)
        return carry

    lax.fori_loop(0, layers, layer_step, 0)
    wait_v(layers * groups)
    wait_k(layers * groups + 1)


def decoder_layers(rows_in, q_first, pos_rows, pos_all, all_k, all_vt, g_attn, w_q, w_o, g_mlp, w_gate, w_up, w_down):
    width = rows_in.shape[1]
    q_width = w_q.shape[2]
    layers = w_q.shape[0]
    return pl.pallas_call(
        layers_kernel,
        out_shape=jax.ShapeDtypeStruct((ROWS, width), jnp.bfloat16),
        in_specs=[SMEM, VMEM, ANY, ANY, ANY, VMEM, VMEM, ANY, ANY, ANY, ANY, ANY, ANY],
        out_specs=VMEM,
        scratch_shapes=[
            pltpu.VMEM((W_SLOTS, width, TILE), jnp.bfloat16),
            pltpu.VMEM((D_SLOTS, TILE, width), jnp.bfloat16),
            pltpu.VMEM((3, SEQ, LANES_STEP), jnp.bfloat16),
            pltpu.VMEM((2, LANES_STEP, SEQ), jnp.bfloat16),
            pltpu.VMEM((ROWS, q_width), jnp.bfloat16),
            pltpu.VMEM((ROWS, width), jnp.bfloat16),
            pltpu.VMEM((ROWS, width), jnp.float32),
            pltpu.VMEM((ROWS, TILE), jnp.bfloat16),
            pltpu.VMEM((ROWS, TILE), jnp.bfloat16),
            pltpu.VMEM((SEQ, PIECE), jnp.float32),
            pltpu.VMEM((2, 2, SEQ // 2, ROWS), jnp.float32),
            pltpu.VMEM((2, 2, SEQ // 2, PIECE), jnp.float32),
            pltpu.VMEM((2, 2, 8, ROWS), jnp.float32),
            pltpu.SMEM((2 * SP,), jnp.int32),
            pltpu.SemaphoreType.DMA((W_SLOTS,)),
            pltpu.SemaphoreType.DMA((D_SLOTS,)),
            pltpu.SemaphoreType.DMA((3,)),
            pltpu.SemaphoreType.DMA((2,)),
            pltpu.SemaphoreType.DMA((2,)),
        ],
        compiler_params=pltpu.CompilerParams(vmem_limit_bytes=VMEM_LIMIT),
        name='layers',
    )(pos_all, pos_rows.reshape(1, ROWS), rows_in, all_k, all_vt, g_attn, g_mlp, w_q, w_o.reshape(layers, q_width, width), w_gate, w_up, w_down, q_first)


def solution(mesh):
    row_spec = P(('dp', 'sp'), None)
    pos_spec = P(('dp', 'sp'))
    full = P()

    def local_step(rows_in, pos_rows, g_kv, w_k, w_v, g_attn, w_q, w_o, g_mlp, w_gate, w_up, w_down):
        all_k, all_vt, pos_all, q_first = gather_kv(rows_in, pos_rows, g_kv, w_k, w_v, g_attn, w_q)
        return decoder_layers(rows_in, q_first, pos_rows, pos_all, all_k, all_vt, g_attn, w_q, w_o, g_mlp, w_gate, w_up, w_down)

    return jax.shard_map(local_step, mesh=mesh, in_specs=(row_spec, pos_spec, full, full, full, full, full, full, full, full, full, full), out_specs=row_spec, check_vma=False)
```
